32 devices in a mesh: shard: 8 (over z, x), grp: 4 (over y, core).
Axes of the slice: x: 2, y: 2, z: 4, core: 2. Of those that a mesh axis runs over, the one named last changes fastest.
Arguments:
- table_t: bfloat16 [100, 622592], P(None, ('shard', 'grp')), may hold values from -6 to 6
- req_rows: int32 [1024, 128], P(('shard', 'grp')), may hold values from 0 to 19455
- count1: int32 [1024], P(('shard', 'grp')), may hold values from 1 to 128, as said below
- frontier_list: int32 [11, 32768], P(None, ('shard', 'grp')), may hold values from 0 to 4095, as said below
- req2_rows: int32 [1024, 128], P(('shard', 'grp')), may hold values from 0 to 1023
- count2: int32 [1024], P(('shard', 'grp')), may hold values from 1 to 128, as said below
- seed_list: int32 [16, 8192], P(None, ('shard', 'grp')), may hold values from 0 to 4095, as said below
- w1_self: bfloat16 [256, 100], replicated, may hold values from -0.625 to 0.625
- w1_neigh: bfloat16 [256, 100], replicated, may hold values from -1.25 to 1.25
- bias1: float32 [256], replicated, may hold values from -3 to 3
- w2_self: bfloat16 [47, 256], replicated, may hold values from -0.375 to 0.375
- w2_neigh: bfloat16 [47, 256], replicated, may hold values from -0.75 to 0.75
- bias2: float32 [47], replicated, may hold values from -3 to 3
Outputs:
- logits: float32 [47, 8192], P(None, ('shard', 'grp'))
The draws below stay inside these ranges and needn't reach their ends.
Inputs may be any that keep to these rules, and one draw needn't show every extreme that they name: count1[r * 32 + o] counts the live slots of the block that device r asks of device o; in every draw some devices are asked for 128 rows by every device. `frontier_list`: every entry o * 128 + j names a live slot (j below count1 of that block) of the asking device. count2[r * 32 + o] counts the live slots of the block that device r asks of device o; in every draw some devices are asked for 128 rows by every device. `seed_list`: every entry o * 128 + j names a live slot (j below count2 of that block) of the asking device.
All inputs are finite; a program needn't handle non-finite values.
Results may differ from the reference program's by a relative error of at most 0.0029.
Values may be sent and summed in bfloat16 or wider, within the bound.
A program may use at most 64 MiB of HBM per device.

```python
import jax
import jax.numpy as jnp
from jax import lax

F = 100
H = 256
C = 47
K1 = 15
K2 = 10
ROWS_DEV = 19456
FRONT_DEV = 1024
SEED_DEV = 256
CAP = 128
CAP2 = 128
NODES = 622592
PAIRS = 1024
N_SHARD = 8
N_GRP = 4
DEVICES = 32


def counts_table(key, capacity):
    first_key, second_key = jax.random.split(key)
    base = jax.random.randint(first_key, (DEVICES, DEVICES), max(1, capacity // 8), capacity // 2 + 1)
    hottest = jax.random.permutation(second_key, DEVICES)[:max(1, DEVICES // 16)]
    is_hot = jnp.any(jnp.arange(DEVICES)[:, None] == hottest[None, :], axis=1)
    return jnp.where(is_hot[None, :], capacity, base).astype(jnp.int32)


def slot_table(key, counts, capacity, entries, per_device):
    first_key, second_key = jax.random.split(key)
    owners = jax.random.randint(first_key, (entries, DEVICES * per_device), 0, DEVICES)
    askers = jnp.broadcast_to((jnp.arange(DEVICES * per_device) // per_device)[None, :], owners.shape)
    live_count = counts[askers, owners]
    offset = jax.random.randint(second_key, owners.shape, 0, 1 << 30) % live_count
    return (owners * capacity + offset).astype(jnp.int32)


def draw_count1(key, part):
    return counts_table(jax.random.fold_in(key, 101), CAP).reshape(-1)


def draw_frontier_list(key, part):
    counts = counts_table(jax.random.fold_in(key, 101), CAP)
    return slot_table(jax.random.fold_in(key, 102), counts, CAP, K2 + 1, FRONT_DEV)


def draw_count2(key, part):
    return counts_table(jax.random.fold_in(key, 201), CAP2).reshape(-1)


def draw_seed_list(key, part):
    counts = counts_table(jax.random.fold_in(key, 201), CAP2)
    return slot_table(jax.random.fold_in(key, 202), counts, CAP2, K1 + 1, SEED_DEV)


def with_ends(values, rng, smallest, top_value):
    shape = values.shape
    index_at = [jax.random.randint(jax.random.fold_in(rng, axis), (), 0, shape[axis]) for axis in range(len(shape))]
    values = values.at[tuple(index_at)].set(smallest)
    longest = shape.index(max(shape))
    index_at[longest] = (index_at[longest] + 1) % shape[longest]
    return values.at[tuple(index_at)].set(top_value)


def block_levels(stream_key, shape, cuts, smallest, largest):
    level, own = 1.0, jax.random.fold_in(stream_key, 6)
    for axis_at, parts in cuts:
        steps = jnp.exp(jax.random.uniform(jax.random.fold_in(own, axis_at), (parts,), jnp.float32, smallest / len(cuts), largest / len(cuts)))
        level = level * jnp.repeat(steps, shape[axis_at] // parts).reshape([-1 if axis == axis_at else 1 for axis in range(len(shape))])
    return level


def gaussian(key, extent, width, most, cuts=(), kind=jnp.bfloat16):
    values = jax.random.normal(key, extent, jnp.float32) * width
    if len(cuts) > 0:
        values = block_levels(key, extent, cuts, -0.22, 0.18) * values
    return jnp.clip(values, min=-most, max=most).astype(kind)


def setup_inputs(seed: int = 0) -> dict:
    streams_of = jax.random.split(jax.random.key(seed), 14)
    table_t = gaussian(streams_of[0], (F, NODES), 1.0, 6.0, ((1, 32),))
    req_rows = with_ends(jax.random.randint(streams_of[1], (PAIRS, CAP), 0, ROWS_DEV), jax.random.fold_in(streams_of[1], 1), 0, ROWS_DEV - 1).astype(jnp.int32)
    count1 = draw_count1(jax.random.fold_in(streams_of[13], 71), 0)
    frontier_list = draw_frontier_list(jax.random.fold_in(streams_of[13], 71), 0)
    req2_rows = with_ends(jax.random.randint(streams_of[4], (PAIRS, CAP2), 0, FRONT_DEV), jax.random.fold_in(streams_of[4], 1), 0, FRONT_DEV - 1).astype(jnp.int32)
    count2 = draw_count2(jax.random.fold_in(streams_of[13], 71), 0)
    seed_list = draw_seed_list(jax.random.fold_in(streams_of[13], 71), 0)
    w1_self = gaussian(streams_of[7], (H, F), F ** -0.5, 0.625)
    w1_neigh = gaussian(streams_of[8], (H, F), (F // 4) ** -0.5, 1.25)
    bias1 = gaussian(streams_of[9], (H,), 0.5, 3.0, (), jnp.float32)
    w2_self = gaussian(streams_of[10], (C, H), H ** -0.5, 0.375)
    w2_neigh = gaussian(streams_of[11], (C, H), (H // 4) ** -0.5, 0.75)
    bias2 = gaussian(streams_of[12], (C,), 0.5, 3.0, (), jnp.float32)
    return dict(table_t=table_t, req_rows=req_rows, count1=count1, frontier_list=frontier_list, req2_rows=req2_rows, count2=count2, seed_list=seed_list, w1_self=w1_self, w1_neigh=w1_neigh, bias1=bias1, w2_self=w2_self, w2_neigh=w2_neigh, bias2=bias2)


def reference(table_t, req_rows, count1, frontier_list, req2_rows, count2, seed_list, w1_self, w1_neigh, bias1, w2_self, w2_neigh, bias2):
    devices = N_SHARD * N_GRP
    table_base = (jnp.arange(devices, dtype=jnp.int32) * ROWS_DEV)[:, None]
    front_base = (jnp.arange(devices, dtype=jnp.int32) * FRONT_DEV)[:, None]
    asked_one = req_rows.reshape(devices, devices, CAP)
    counts_one = count1.reshape(devices, devices)
    lists_one = frontier_list.reshape(K2 + 1, devices, FRONT_DEV).transpose(1, 0, 2)

    def layer_one(args):
        wanted, counts, picks = args
        columns = jnp.take(table_t, (wanted + table_base).reshape(-1).astype(jnp.int32), axis=1)
        is_live = (jnp.arange(CAP, dtype=jnp.int32)[None, :] < counts[:, None]).reshape(-1)
        columns = jnp.where(is_live[None, :], columns, jnp.zeros((), columns.dtype))
        picked = jnp.take(columns, picks.reshape(-1), axis=1).reshape(F, K2 + 1, FRONT_DEV)
        summed = (jnp.sum(picked[:, 1:].astype(jnp.float32), axis=1) / K2).astype(jnp.bfloat16)
        preact = jnp.dot(w1_self, picked[:, 0], preferred_element_type=jnp.float32)
        preact = preact + jnp.dot(w1_neigh, summed, preferred_element_type=jnp.float32) + bias1[:, None]
        return jax.nn.relu(preact).astype(jnp.bfloat16)

    hidden = lax.map(layer_one, (asked_one, counts_one, lists_one))
    hidden = hidden.transpose(1, 0, 2).reshape(H, devices * FRONT_DEV)
    asked_two = req2_rows.reshape(devices, devices, CAP2)
    counts_two = count2.reshape(devices, devices)
    lists_two = seed_list.reshape(K1 + 1, devices, SEED_DEV).transpose(1, 0, 2)

    def layer_two(args):
        wanted, counts, picks = args
        columns = jnp.take(hidden, (wanted + front_base).reshape(-1).astype(jnp.int32), axis=1)
        is_live = (jnp.arange(CAP2, dtype=jnp.int32)[None, :] < counts[:, None]).reshape(-1)
        columns = jnp.where(is_live[None, :], columns, jnp.zeros((), columns.dtype))
        picked = jnp.take(columns, picks.reshape(-1), axis=1).reshape(H, K1 + 1, SEED_DEV)
        near = jnp.sum(picked[:, 1:].astype(jnp.float32), axis=1) / K1
        result = jnp.dot(w2_self, picked[:, 0], preferred_element_type=jnp.float32)
        result = result + jnp.dot(w2_neigh.astype(jnp.float32), near, precision=lax.Precision.HIGHEST, preferred_element_type=jnp.float32)
        return result + bias2[:, None]

    logits = lax.map(layer_two, (asked_two, counts_two, lists_two))
    return logits.transpose(1, 0, 2).reshape(C, devices * SEED_DEV)
```

```python
import functools

import jax
import jax.numpy as jnp
from jax import lax
from jax.experimental import pallas as pl
from jax.experimental.pallas import tpu as pltpu
from jax.sharding import PartitionSpec as P

AXES = ("shard", "grp")
LANES = 128
MIB = 1024 * 1024
MATRIX_LIMIT = 4 * MIB
EARLY = 5
GROUPS = (0, 16, 24, 30, 32)
LAG = 4


FIELDS = 8
FIELD_BITS = 4


def tile(i, size=LANES):
    return pl.ds(pl.multiple_of(i * size, size), size)


def dot32(a, b):
    return jnp.dot(a, b, preferred_element_type=jnp.float32)


def tile_names(span):
    first = lax.broadcasted_iota(jnp.int32, (16, LANES), 0).astype(jnp.float32)
    return [(first + float(16 * b)).astype(jnp.bfloat16) for b in range(span // 16)]


def hits(row, names):
    few = jnp.broadcast_to(row, (16, row.shape[1])).astype(jnp.bfloat16)
    one, zero = jnp.ones((), jnp.bfloat16), jnp.zeros((), jnp.bfloat16)
    return [jnp.where(few == name, one, zero) for name in names]


def prepare_list(list_ref, key_ref, unit_ref, first_ref, cap):
    words = cap // FIELDS
    entry = list_ref[...]
    owner, slot = entry >> (cap.bit_length() - 1), entry & (cap - 1)
    key_ref[...] = owner * words + (slot & (words - 1))
    unit_ref[...] = jnp.ones((), jnp.int32) << (FIELD_BITS * (slot >> (words.bit_length() - 1)))
    first_ref[...] = entry[0:1].astype(jnp.float32)


def count_tile(key_ref, unit_ref, first, name, names, own_ref, near_ref, own_at, near_at, cols):
    words = name.shape[0]
    total = jnp.zeros(name.shape, jnp.int32)
    for k in range(1, key_ref.shape[0]):
        total = total + jnp.where(key_ref[k : k + 1, cols] == name, unit_ref[k : k + 1, cols], 0)
    for b in range(FIELDS):
        field = (total >> (FIELD_BITS * b)) & (2**FIELD_BITS - 1)
        near_ref[pl.ds(pl.multiple_of(near_at + b * words, words), words), cols] = field.astype(
            jnp.float32
        ).astype(jnp.bfloat16)
    for b, part in enumerate(hits(first, names)):
        own_ref[pl.ds(pl.multiple_of(own_at + b * 16, 16), 16), cols] = part


def count_slots(key_ref, unit_ref, first_ref, own_ref, near_ref, cap, owner_of, first, last):
    across = key_ref.shape[1] // LANES
    some = 4 if across % 4 == 0 else 1
    words = cap // FIELDS
    names = tile_names(cap)
    low = lax.broadcasted_iota(jnp.int32, (words, LANES), 0)

    def one(i, carry):
        at, base = lax.div(i, across // some), lax.rem(i, across // some) * some
        owner = owner_of(at)
        name, start = low + owner * words, (owner * cap).astype(jnp.float32)
        for c in range(some):
            cols = tile(base + c)
            own = first_ref[0:1, cols] - start
            count_tile(
                key_ref, unit_ref, own, name, names, own_ref, near_ref, at * cap, at * cap, cols
            )
        return carry

    lax.fori_loop(first * (across // some), last * (across // some), one, 0)


def select_seeds(lists_ref, key_ref, unit_ref, first_ref, out_ref, me, cap, first, last):
    seeds = lists_ref.shape[3]
    words = cap // FIELDS
    names = tile_names(cap)
    low = lax.broadcasted_iota(jnp.int32, (words, LANES), 0)

    def one(t, carry):
        local = lists_ref[lax.rem(t, 2), lax.div(t, 2)].astype(jnp.int32) - me * cap
        field = local >> (words.bit_length() - 1)
        here = jnp.logical_and(field >= 0, field < FIELDS)
        key_ref[...] = local & (words - 1)
        unit_ref[...] = jnp.where(here, jnp.ones((), jnp.int32) << (FIELD_BITS * (field & (FIELDS - 1))), 0)
        first_ref[...] = local[0:1].astype(jnp.float32)
        for c in range(seeds // LANES):
            cols = slice(c * LANES, (c + 1) * LANES)
            at = t * 2 * cap
            count_tile(
                key_ref, unit_ref, first_ref[0:1, cols], low, names, out_ref, out_ref, at, at + cap, cols
            )
        return carry

    lax.fori_loop(first, last, one, 0)


def onehot_slots(asked_ref, out_ref, cap, first, last):
    nodes = out_ref.shape[0]
    names = tile_names(LANES)

    def one(t, carry):
        wanted = asked_ref[t, 1:2].astype(jnp.float32)
        for b in range(nodes // LANES):
            for c, part in enumerate(hits(wanted - float(b * LANES), names)):
                out_ref[b * LANES + 16 * c : b * LANES + 16 * c + 16, tile(t, cap)] = part
        return carry

    lax.fori_loop(first, last, one, 0)


def whole_kernel(grp, rows_two, *refs):
    req_hbm, req2_hbm, front_hbm, seed_hbm, w1s_hbm, w2s_hbm = (refs[k] for k in (1, 2, 5, 6, 7, 10))
    devices, cap, cap_two = req_hbm.shape[0], req_hbm.shape[2], req2_hbm.shape[2]
    nodes, seeds = front_hbm.shape[1], seed_hbm.shape[1]
    width, hidden_width = w1s_hbm.shape
    wide = -(-width // LANES) * LANES
    bf16 = jnp.bfloat16
    pl.run_scoped(
        functools.partial(inner_kernel, grp, *refs),
        pltpu.VMEM((hidden_width, 2 * wide), bf16),
        pltpu.VMEM((rows_two, hidden_width), bf16),
        pltpu.VMEM((devices * cap, nodes), bf16),
        pltpu.VMEM((devices * cap, nodes), bf16),
        pltpu.VMEM((nodes, devices * cap_two), bf16),
        pltpu.VMEM((2 * devices * cap_two, seeds), bf16),
        pltpu.VMEM((-(-width // 16) * 16, devices * cap), bf16),
        pltpu.VMEM((2 * wide, nodes), bf16),
        pltpu.VMEM((rows_two, nodes), bf16),
        pltpu.VMEM((2, 2, rows_two // 2, 2 * cap_two), bf16),
    )


def inner_kernel(
    grp,
    table_hbm,
    req_hbm,
    req2_hbm,
    count1_hbm,
    count2_hbm,
    front_hbm,
    seed_hbm,
    w1s_hbm,
    w1n_hbm,
    bias1_hbm,
    w2s_hbm,
    w2n_hbm,
    out_ref,
    table,
    req_ref,
    req2_ref,
    count1_ref,
    count2_ref,
    front_ref,
    seed_ref,
    w1s_ref,
    w1n_ref,
    bias1_ref,
    w2s_ref,
    w2n_ref,
    key1,
    unit1,
    first1,
    key2,
    unit2,
    first2,
    ask_out,
    asked,
    ids,
    rows,
    block,
    send,
    got,
    list_out,
    lists,
    acc,
    term_out,
    term_in,
    term,
    send2,
    got2,
    load_sems,
    ids_sem,
    out_sems,
    in_sems,
    group_sems,
    cross_sems,
    w1,
    w2,
    own,
    near,
    onehot,
    select,
    flat,
    pair,
    payload,
    chosen,
):
    devices, _, cap = req_ref.shape
    cap_two = req2_ref.shape[2]
    me = lax.axis_index(AXES[0]) * grp + lax.axis_index(AXES[1])
    half = devices // 2
    bits = devices.bit_length() - 1

    def peer(t):
        total = 0
        for i in range(bits):
            mine = lax.rem(lax.div(me, 2**i), 2)
            if isinstance(t, int):
                bit = 1 - mine if (t >> i) & 1 else mine
            else:
                other = lax.rem(lax.div(t, 2**i), 2)
                bit = mine + other - 2 * mine * other
            total = total + bit * 2**i
        return total

    def step_of(p):
        return half * (1 - lax.rem(p, 2)) + lax.div(p, 2)

    def coordinates(to):
        return (lax.div(to, grp), lax.rem(to, grp))

    def place(t):
        return coordinates(peer(t))

    def remote(src, dst, out_sem, in_sem, to):
        return pltpu.make_async_remote_copy(
            src_ref=src,
            dst_ref=dst,
            send_sem=out_sem,
            recv_sem=in_sem,
            device_id=coordinates(to),
            device_id_type=pl.DeviceIdType.MESH,
        )

    steps = [devices * k // 32 for k in GROUPS]

    def group_of(p):
        return sum((p >= edge) * 1 if isinstance(p, int) else (p >= edge).astype(jnp.int32) for edge in steps[1:-1])

    def feature(to, t, p):
        return remote(send.at[t], got.at[p], out_sems.at[1], group_sems.at[group_of(p)], to)

    def arrived(first, last):
        count = last - first - (first <= 1 < last)
        remote(
            send.at[pl.ds(0, count)],
            got.at[pl.ds(0, count)],
            out_sems.at[1],
            group_sems.at[group_of(first)],
            peer(1),
        ).wait_recv()

    pairs = (
        (front_hbm, front_ref),
        (req_hbm, req_ref),
        (req2_hbm, req2_ref),
        (table_hbm, table),
        (w1s_hbm, w1s_ref),
        (w1n_hbm, w1n_ref),
        (bias1_hbm, bias1_ref),
        (w2s_hbm, w2s_ref),
        (w2n_hbm, w2n_ref),
        (seed_hbm, seed_ref),
        (count1_hbm, count1_ref),
        (count2_hbm, count2_ref),
    )
    loads = [pltpu.make_async_copy(a, b, load_sems.at[i]) for i, (a, b) in enumerate(pairs)]
    for load in loads[:4]:
        load.start()
    barrier = pltpu.get_barrier_semaphore()
    for t in range(devices - 1, 0, -1):
        pl.semaphore_signal(
            barrier, inc=1, device_id=place(t), device_id_type=pl.DeviceIdType.MESH
        )
    for load in loads[4:]:
        load.start()
    loads[0].wait()
    prepare_list(front_ref, key1, unit1, first1, cap)
    loads[1].wait()
    loads[2].wait()
    ask_out[:, 0:1, :] = req_ref[...]
    ask_out[:, 1:2, :] = req2_ref[...]
    early = devices * EARLY // 32

    def owner_at(p):
        return peer(step_of(p))

    count_slots(key1, unit1, first1, own, near, cap, owner_at, 0, early)
    pl.semaphore_wait(barrier, devices - 1)

    couples = devices // 2

    def ask(t):
        return remote(ask_out.at[peer(t)], asked.at[t], out_sems.at[0], in_sems.at[0], peer(t))

    def give(i):
        return remote(list_out, lists.at[0, i], out_sems.at[2], in_sems.at[1], peer(2 * i))

    def hand_on():
        return remote(lists.at[0], lists.at[1], out_sems.at[3], in_sems.at[2], peer(1))

    for t in range(devices - 1, 0, -1):
        ask(t).start()
    asked[0] = ask_out[me]
    for load in loads[3:9]:
        load.wait()
    width, hidden_width = w1s_ref.shape[0], w1.shape[0]
    wide = w1.shape[1] // 2
    classes, half_rows = w2s_ref.shape[0], w2.shape[0] // 2
    w1[...] = jnp.zeros_like(w1)
    w1[:, :width] = w1s_ref[...].T
    w1[:, wide : wide + width] = w1n_ref[...].T
    w2[...] = jnp.zeros_like(w2)
    w2[:classes] = w2s_ref[...]
    w2[half_rows : half_rows + classes] = w2n_ref[...]
    pair[...] = jnp.zeros_like(pair)
    bias1 = jnp.broadcast_to(bias1_ref[...], (8, hidden_width)).T[:, :1]

    step = 4 * LANES if rows.shape[0] % (4 * LANES) == 0 else LANES

    def transpose(i, carry):
        rows[tile(i, step), :] = table[:, tile(i, step)].T.astype(jnp.float32)
        return carry

    pieces = rows.shape[0] // step
    lax.fori_loop(0, pieces // 2, transpose, 0)
    for load in loads[9:]:
        load.wait()
    entry = seed_ref[...]
    owner, slot = entry >> (cap_two.bit_length() - 1), entry & (cap_two - 1)

    def limit_of(o, limit):
        return jnp.where(owner == o, count2_ref[o], limit)

    live = slot < lax.fori_loop(0, devices, limit_of, jnp.zeros_like(entry))
    list_out[...] = jnp.where(live, entry, -1).astype(list_out.dtype)
    lists[0, 0] = list_out[...]
    for i in range(couples - 1, 0, -1):
        give(i).start()
    lax.fori_loop(pieces // 2, pieces * 3 // 4, transpose, 0)
    remote(ask_out.at[pl.ds(0, devices - 1)], asked.at[pl.ds(1, devices - 1)], out_sems.at[0], in_sems.at[0], peer(1)).wait()
    to_scalars = pltpu.make_async_copy(asked, ids, ids_sem)
    to_scalars.start()
    lax.fori_loop(pieces * 3 // 4, pieces, transpose, 0)
    to_scalars.wait()

    def pick(t, at):
        for j in range(cap):
            block[at, j : j + 1, :] = rows[pl.ds(ids[t, 0, j], 1), :]
        return block[at].T.astype(jnp.bfloat16)

    def pick_and_send(i, carry):
        to, before = peer(i), peer(i - 1)
        send[half + i] = pick(half + i, 0)
        send[i] = pick(i, 1)
        feature(lax.rem(before + half, devices), half + i - 1, 2 * i - 2).start()
        feature(before, i - 1, 2 * i - 1).start()
        return carry

    send[half] = pick(half, 0)
    got[1] = pick(0, 1)
    send[half + 1] = pick(half + 1, 0)
    feature(peer(half), half, 0).start()
    send[1] = pick(1, 1)
    lax.fori_loop(2, half, pick_and_send, 0)
    onehot_slots(asked, onehot, cap_two, 0, 2)
    feature(peer(devices - 1), devices - 1, devices - 2).start()
    feature(peer(half - 1), half - 1, devices - 1).start()
    onehot_slots(asked, onehot, cap_two, 2, devices)
    remote(lists.at[0, pl.ds(0, couples - 1)], lists.at[0, pl.ds(1, couples - 1)], out_sems.at[2], in_sems.at[1], peer(1)).wait()
    hand_on().start()
    count_slots(key1, unit1, first1, own, near, cap, owner_at, early, devices)
    hand_on().wait()
    select_seeds(lists, key2, unit2, first2, select, me, cap_two, 0, devices)
    nodes = own.shape[1]
    chunk = 2 * LANES
    def lay(p, carry):
        slot = lax.broadcasted_iota(jnp.int32, got.shape[1:], 1)
        live = jnp.where(slot < count1_ref[owner_at(p)], got[p].astype(jnp.float32), 0.0)
        flat[:width, tile(p, cap)] = live.astype(jnp.bfloat16)
        return carry

    def arrive(first, last):
        arrived(first, last)
        lax.fori_loop(first, last, lay, 0)

    arrive(0, steps[1])

    def add_up(first, last, fresh):
        for c in range(nodes // chunk):
            cols = slice(c * chunk, (c + 1) * chunk)
            for m, matrix in enumerate((own, near)):
                part = dot32(flat[:width, first * cap : last * cap], matrix[first * cap : last * cap, cols])
                acc[m, :, cols] = part if fresh else acc[m, :, cols] + part

    add_up(0, steps[1], True)
    for first, last in zip(steps[1:-2], steps[2:-1]):
        arrive(first, last)
        add_up(first, last, False)
    fan_two, fan_one = 1.0 / (front_ref.shape[0] - 1), 1.0 / (seed_ref.shape[0] - 1)
    arrive(steps[-2], steps[-1])
    tail = slice(steps[-2] * cap, steps[-1] * cap)
    scale = jnp.where(lax.broadcasted_iota(jnp.int32, (w2.shape[0], 1), 0) < half_rows, 1.0, fan_one)
    for c in range(nodes // chunk):
        cols = slice(c * chunk, (c + 1) * chunk)
        mine = acc[0, :, cols] + dot32(flat[:width, tail], own[tail, cols])
        summed = (acc[1, :, cols] + dot32(flat[:width, tail], near[tail, cols])) * fan_two
        pair[:width, cols] = mine.astype(jnp.bfloat16)
        pair[wide : wide + width, cols] = summed.astype(jnp.bfloat16)
    for c in range(nodes // chunk):
        cols = slice(c * chunk, (c + 1) * chunk)
        preact = dot32(w1[...], pair[:, cols]) + bias1
        hidden = jnp.maximum(preact, 0.0).astype(jnp.bfloat16)
        payload[:, cols] = (dot32(w2[...], hidden) * scale).astype(jnp.bfloat16)
    def couple_of(s):
        if isinstance(s, int):
            return 0 if s == couples - 1 else 1 + (s + couples // 2 - 1) % (couples - 1)
        return 1 + lax.rem(s + couples // 2 - 1, couples - 1)

    def choose(i, at):
        both = dot32(payload[...], onehot[:, tile(i, 2 * cap_two)]).astype(jnp.bfloat16)
        for c in range(2):
            cols = slice(c * cap_two, (c + 1) * cap_two)
            chosen[at, c, :, :cap_two] = both[:half_rows, cols]
            chosen[at, c, :, cap_two:] = both[half_rows:, cols]

    def terms(i, at):
        term[i] = dot32(chosen[at, 0], select[tile(2 * i, 2 * cap_two), :])
        term_out[i] = dot32(chosen[at, 1], select[tile(2 * i + 1, 2 * cap_two), :])

    def cross(s):
        i = couple_of(s)
        return remote(term_out.at[i], term_in.at[i], out_sems.at[4], cross_sems.at[i], peer(1))

    def join(s):
        cross(s).wait_recv()
        i = couple_of(s)
        send2[i] = (term[i] + term_in[i]).astype(jnp.bfloat16)

    def away(s):
        i = couple_of(s)
        return remote(send2.at[i], got2.at[i], out_sems.at[5], in_sems.at[3], peer(2 * i))

    def steady(s, carry, far=True):
        at = s % 2 if isinstance(s, int) else lax.rem(s, 2)
        terms(couple_of(s), at)
        if not isinstance(s, int) or s < couples - 1:
            choose(couple_of(s + 1), 1 - at)
        if not isinstance(s, int) or s >= 1:
            cross(s - 1).start()
        if not isinstance(s, int) or s >= LAG:
            join(s - LAG)
        if not isinstance(s, int) or s > LAG:
            away(s - LAG - 1).start()
        return carry

    choose(couple_of(0), 0)
    for s in range(LAG + 1):
        steady(s, 0)
    lax.fori_loop(LAG + 1, couples - 2, steady, 0)
    steady(couples - 2, 0)
    steady(couples - 1, 0)
    cross(couples - 1).start()
    for s in range(couples - LAG, couples):
        if s < couples - 1:
            join(s)
        else:
            cross(s).wait_recv()
        away(s - 1).start()
    total = term[0] + term_in[0]
    for src, dst, k in ((send, got, 1), (term_out, term_in, 4), (send2, got2, 5)):
        sent = src.shape[0] - (k != 4)
        whole = remote(src.at[pl.ds(0, sent)], dst.at[pl.ds(0, sent)], out_sems.at[k], in_sems.at[3], peer(1))
        if k == 5:
            whole.wait()
        else:
            whole.wait_send()
    for i in range(1, couples):
        total = total + got2[i].astype(jnp.float32)
    out_ref[...] = total[:classes]


def mask_rows(received, counts, capacity):
    is_live = (jnp.arange(capacity, dtype=jnp.int32)[None, :] < counts[:, None]).reshape(-1)
    flat = received.reshape(-1, received.shape[-1])
    return jnp.where(is_live[:, None], flat, jnp.zeros((), flat.dtype))


def right_product(rows, weight):
    return lax.dot_general(
        rows, weight, (((1,), (1,)), ((), ())), preferred_element_type=jnp.float32
    )


def take_body(
    table_t,
    req_rows,
    count1,
    frontier_list,
    req2_rows,
    count2,
    seed_list,
    w1_self,
    w1_neigh,
    bias1,
    w2_self,
    w2_neigh,
    bias2,
):
    feat_width = table_t.shape[0]
    capacity = req_rows.shape[1]
    table_rows = table_t.T
    picked_rows = jnp.take(
        table_rows,
        lax.all_to_all(req_rows, AXES, split_axis=0, concat_axis=0, tiled=True),
        axis=0,
    )
    received = lax.all_to_all(
        picked_rows, AXES, split_axis=0, concat_axis=0, tiled=True
    )
    flat = mask_rows(received, count1, capacity)
    fanout_two = frontier_list.shape[0] - 1
    front_nodes = frontier_list.shape[1]
    picked = jnp.take(flat, frontier_list.reshape(-1), axis=0).reshape(
        fanout_two + 1, front_nodes, feat_width
    )
    summed = (jnp.sum(picked[1:].astype(jnp.float32), axis=0) / fanout_two).astype(jnp.bfloat16)
    preact = right_product(picked[0], w1_self) + right_product(summed, w1_neigh) + bias1[None, :]
    hidden_rows = jax.nn.relu(preact).astype(jnp.bfloat16)
    cap_two = req2_rows.shape[1]
    payload = jnp.concatenate(
        [right_product(hidden_rows, w2_self), right_product(hidden_rows, w2_neigh)], axis=1
    )
    chosen = jnp.take(
        payload,
        lax.all_to_all(req2_rows, AXES, split_axis=0, concat_axis=0, tiled=True),
        axis=0,
    )
    got_back = lax.all_to_all(chosen, AXES, split_axis=0, concat_axis=0, tiled=True)
    flat_two = mask_rows(got_back, count2, cap_two)
    fanout_one = seed_list.shape[0] - 1
    seed_nodes = seed_list.shape[1]
    picked_two = jnp.take(flat_two, seed_list.reshape(-1), axis=0).reshape(
        fanout_one + 1, seed_nodes, flat_two.shape[1]
    )
    classes = w2_self.shape[0]
    near = jnp.sum(picked_two[1:, :, classes:], axis=0) / fanout_one
    logits = (picked_two[0, :, :classes] + near).T + bias2[:, None]
    return logits


def body(
    table_t,
    req_rows,
    count1,
    frontier_list,
    req2_rows,
    count2,
    seed_list,
    w1_self,
    w1_neigh,
    bias1,
    w2_self,
    w2_neigh,
    bias2,
):
    devices, cap = req_rows.shape
    cap_two = req2_rows.shape[1]
    nodes = frontier_list.shape[1]
    small = devices * max(cap, cap_two) * nodes <= MATRIX_LIMIT
    even = devices >= 32 and devices & (devices - 1) == 0
    plain = cap == cap_two == LANES and nodes % (2 * LANES) == 0
    few = max(frontier_list.shape[0], seed_list.shape[0]) <= 2**FIELD_BITS
    if not (small and even and plain and few):
        return take_body(
            table_t,
            req_rows,
            count1,
            frontier_list,
            req2_rows,
            count2,
            seed_list,
            w1_self,
            w1_neigh,
            bias1,
            w2_self,
            w2_neigh,
            bias2,
        )
    width, table_rows = table_t.shape
    entries, entries_two = frontier_list.shape[0], seed_list.shape[0]
    seeds = seed_list.shape[1]
    hidden_width, classes = w1_self.shape[0], w2_self.shape[0]
    rows_two = 2 * (-(-classes // 16) * 16)
    bf16, f32, i32 = jnp.bfloat16, jnp.float32, jnp.int32
    logits = pl.pallas_call(
        functools.partial(whole_kernel, lax.axis_size(AXES[1]), rows_two),
        in_specs=[pl.BlockSpec(memory_space=pl.ANY)] * 12,
        out_specs=pl.BlockSpec(memory_space=pltpu.VMEM),
        out_shape=jax.ShapeDtypeStruct((classes, seeds), f32),
        scratch_shapes=[
            pltpu.VMEM((width, table_rows), bf16),
            pltpu.VMEM((devices, 1, cap), i32),
            pltpu.VMEM((devices, 1, cap_two), i32),
            pltpu.SMEM((devices,), i32),
            pltpu.SMEM((devices,), i32),
            pltpu.VMEM((entries, nodes), i32),
            pltpu.VMEM((entries_two, seeds), i32),
            pltpu.VMEM((width, hidden_width), bf16),
            pltpu.VMEM((width, hidden_width), bf16),
            pltpu.VMEM((1, hidden_width), f32),
            pltpu.VMEM((classes, hidden_width), bf16),
            pltpu.VMEM((classes, hidden_width), bf16),
            pltpu.VMEM((entries, nodes), i32),
            pltpu.VMEM((entries, nodes), i32),
            pltpu.VMEM((1, nodes), f32),
            pltpu.VMEM((entries_two, seeds), i32),
            pltpu.VMEM((entries_two, seeds), i32),
            pltpu.VMEM((1, seeds), f32),
            pltpu.VMEM((devices, 2, cap), i32),
            pltpu.VMEM((devices, 2, cap), i32),
            pltpu.SMEM((devices, 2, cap), i32),
            pltpu.VMEM((table_rows, width), f32),
            pltpu.VMEM((2, cap, width), f32),
            pltpu.VMEM((devices, width, cap), bf16),
            pltpu.VMEM((devices, width, cap), bf16),
            pltpu.VMEM((entries_two, seeds), jnp.int16),
            pltpu.VMEM((2, devices // 2, entries_two, seeds), jnp.int16),
            pltpu.VMEM((2, width, nodes), f32),
            pltpu.VMEM((devices // 2, rows_two // 2, seeds), f32),
            pltpu.VMEM((devices // 2, rows_two // 2, seeds), f32),
            pltpu.VMEM((devices // 2, rows_two // 2, seeds), f32),
            pltpu.VMEM((devices // 2, rows_two // 2, seeds), bf16),
            pltpu.VMEM((devices // 2, rows_two // 2, seeds), bf16),
            pltpu.SemaphoreType.DMA((12,)),
            pltpu.SemaphoreType.DMA,
            pltpu.SemaphoreType.DMA((6,)),
            pltpu.SemaphoreType.DMA((4,)),
            pltpu.SemaphoreType.DMA((len(GROUPS) - 1,)),
            pltpu.SemaphoreType.DMA((devices // 2,)),
        ],
        compiler_params=pltpu.CompilerParams(
            vmem_limit_bytes=63 * MIB, collective_id=0, has_side_effects=True
        ),
    )(
        table_t,
        req_rows[:, None, :],
        req2_rows[:, None, :],
        count1,
        count2,
        frontier_list,
        seed_list,
        w1_self.T,
        w1_neigh.T,
        bias1[None, :],
        w2_self,
        w2_neigh,
    )
    return logits + bias2[:, None]


def solution(mesh):
    in_specs = (
        P(None, AXES),
        P(AXES, None),
        P(AXES),
        P(None, AXES),
        P(AXES, None),
        P(AXES),
        P(None, AXES),
        P(),
        P(),
        P(),
        P(),
        P(),
        P(),
    )
    return jax.shard_map(
        body, mesh=mesh, in_specs=in_specs, out_specs=P(None, AXES), check_vma=False
    )
```

```python
import functools

import jax
import jax.numpy as jnp
from jax import lax
from jax.experimental import pallas as pl
from jax.experimental.pallas import tpu as pltpu
from jax.sharding import PartitionSpec as P

AXES = ("shard", "grp")
LANES = 128
MIB = 1024 * 1024
MATRIX_LIMIT = 4 * MIB
EARLY = 2
GROUPS = (0, 16, 24, 30, 32)
BRIDGE = 2


FIELDS = 8
FIELD_BITS = 4


def tile(i, size=LANES):
    return pl.ds(pl.multiple_of(i * size, size), size)


def dot32(a, b):
    return jnp.dot(a, b, preferred_element_type=jnp.float32)


def tile_names(span):
    first = lax.broadcasted_iota(jnp.int32, (16, LANES), 0).astype(jnp.float32)
    return [(first + float(16 * b)).astype(jnp.bfloat16) for b in range(span // 16)]


def hits(row, names):
    few = jnp.broadcast_to(row, (16, row.shape[1])).astype(jnp.bfloat16)
    one, zero = jnp.ones((), jnp.bfloat16), jnp.zeros((), jnp.bfloat16)
    return [jnp.where(few == name, one, zero) for name in names]


def prepare_list(list_ref, key_ref, unit_ref, first_ref, cap):
    words = cap // FIELDS
    entry = list_ref[...]
    owner, slot = entry >> (cap.bit_length() - 1), entry & (cap - 1)
    key_ref[...] = owner * words + (slot & (words - 1))
    unit_ref[...] = jnp.ones((), jnp.int32) << (FIELD_BITS * (slot >> (words.bit_length() - 1)))
    first_ref[...] = entry[0:1].astype(jnp.float32)


def count_tile(key_ref, unit_ref, first, name, names, own_ref, near_ref, own_at, near_at, cols, to):
    words = name.shape[0]
    total = jnp.zeros(name.shape, jnp.int32)
    for k in range(1, key_ref.shape[0]):
        total = total + jnp.where(key_ref[k : k + 1, cols] == name, unit_ref[k : k + 1, cols], 0)
    for b in range(FIELDS):
        field = (total >> (FIELD_BITS * b)) & (2**FIELD_BITS - 1)
        near_ref[to, pl.ds(pl.multiple_of(near_at + b * words, words), words), :] = field.astype(
            jnp.float32
        ).astype(jnp.bfloat16)
    for b, part in enumerate(hits(first, names)):
        own_ref[to, pl.ds(pl.multiple_of(own_at + b * 16, 16), 16), :] = part


def count_slots(key_ref, unit_ref, first_ref, own_ref, near_ref, cap, owner_of, first, last):
    across = key_ref.shape[1] // LANES
    some = 4 if across % 4 == 0 else 1
    words = cap // FIELDS
    names = tile_names(cap)
    low = lax.broadcasted_iota(jnp.int32, (words, LANES), 0)

    def one(i, carry):
        at, base = lax.div(i, across // some), lax.rem(i, across // some) * some
        owner = owner_of(at)
        name, start = low + owner * words, (owner * cap).astype(jnp.float32)
        for c in range(some):
            cols = tile(base + c)
            own = first_ref[0:1, cols] - start
            count_tile(
                key_ref, unit_ref, own, name, names, own_ref, near_ref, at * cap, at * cap, cols, base + c
            )
        return carry

    lax.fori_loop(first * (across // some), last * (across // some), one, 0)


def select_seeds(lists_ref, key_ref, unit_ref, first_ref, out_ref, me, cap, first, last):
    seeds = lists_ref.shape[3]
    words = cap // FIELDS
    names = tile_names(cap)
    low = lax.broadcasted_iota(jnp.int32, (words, LANES), 0)

    def one(t, carry):
        local = lists_ref[lax.rem(t, 2), lax.div(t, 2)].astype(jnp.int32) - me * cap
        field = local >> (words.bit_length() - 1)
        here = jnp.logical_and(field >= 0, field < FIELDS)
        key_ref[...] = local & (words - 1)
        unit_ref[...] = jnp.where(here, jnp.ones((), jnp.int32) << (FIELD_BITS * (field & (FIELDS - 1))), 0)
        first_ref[...] = local[0:1].astype(jnp.float32)
        for c in range(seeds // LANES):
            cols = slice(c * LANES, (c + 1) * LANES)
            to = t * (seeds // LANES) + c
            count_tile(
                key_ref, unit_ref, first_ref[0:1, cols], low, names, out_ref, out_ref, 0, cap, cols, to
            )
        return carry

    lax.fori_loop(first, last, one, 0)


def onehot_slots(asked_ref, out_ref, cap, first, last):
    nodes = out_ref.shape[1]
    names = tile_names(LANES)

    def one(t, carry):
        wanted = asked_ref[t].astype(jnp.float32)
        for b in range(nodes // LANES):
            for c, part in enumerate(hits(wanted - float(b * LANES), names)):
                out_ref[t, b * LANES + 16 * c : b * LANES + 16 * c + 16, :] = part
        return carry

    lax.fori_loop(first, last, one, 0)


def whole_kernel(grp, rows_two, *refs):
    req_hbm, req2_hbm, front_hbm, seed_hbm, w1s_hbm, w2s_hbm = (refs[k] for k in (1, 2, 5, 6, 7, 10))
    devices, cap, cap_two = req_hbm.shape[0], req_hbm.shape[2], req2_hbm.shape[2]
    nodes, seeds = front_hbm.shape[1], seed_hbm.shape[1]
    width, hidden_width = w1s_hbm.shape
    wide = -(-width // LANES) * LANES
    bf16 = jnp.bfloat16
    pl.run_scoped(
        functools.partial(inner_kernel, grp, *refs),
        pltpu.VMEM((hidden_width, 2 * wide), bf16),
        pltpu.VMEM((rows_two, hidden_width), bf16),
        pltpu.VMEM((nodes // LANES, devices * cap, LANES), bf16),
        pltpu.VMEM((nodes // LANES, devices * cap, LANES), bf16),
        pltpu.VMEM((devices, nodes, LANES), bf16),
        pltpu.VMEM((devices * seeds // LANES, 2 * cap_two, LANES), bf16),
        pltpu.VMEM((devices, -(-width // 16) * 16, cap), bf16),
        pltpu.VMEM((nodes // LANES, 2 * wide, LANES), bf16),
        pltpu.VMEM((nodes // LANES, rows_two, LANES), bf16),
        pltpu.VMEM((devices // 2, 2, rows_two // 2, 2 * cap_two), bf16),
    )


def inner_kernel(
    grp,
    table_hbm,
    req_hbm,
    req2_hbm,
    count1_hbm,
    count2_hbm,
    front_hbm,
    seed_hbm,
    w1s_hbm,
    w1n_hbm,
    bias1_hbm,
    w2s_hbm,
    w2n_hbm,
    out_ref,
    table,
    req_ref,
    req2_ref,
    count1_ref,
    count2_ref,
    front_ref,
    seed_ref,
    w1s_ref,
    w1n_ref,
    bias1_ref,
    w2s_ref,
    w2n_ref,
    key1,
    unit1,
    first1,
    key2,
    unit2,
    first2,
    asked,
    ids,
    rows,
    block,
    send,
    got,
    list_out,
    lists,
    acc,
    term_out,
    term_in,
    term,
    send2,
    got2,
    bridge_out,
    bridge_in,
    load_sems,
    ids_sem,
    out_sems,
    in_sems,
    group_sems,
    cross_sems,
    bridge_sems,
    w1,
    w2,
    own,
    near,
    onehot,
    select,
    flat,
    pair,
    payload,
    chosen,
):
    devices, _, cap = req_ref.shape
    cap_two = req2_ref.shape[2]
    me = lax.axis_index(AXES[0]) * grp + lax.axis_index(AXES[1])
    half = devices // 2
    bits = devices.bit_length() - 1

    def peer(t):
        total = 0
        for i in range(bits):
            mine = lax.rem(lax.div(me, 2**i), 2)
            if isinstance(t, int):
                bit = 1 - mine if (t >> i) & 1 else mine
            else:
                other = lax.rem(lax.div(t, 2**i), 2)
                bit = mine + other - 2 * mine * other
            total = total + bit * 2**i
        return total

    def step_of(p):
        return half * (1 - lax.rem(p, 2)) + lax.div(p, 2)

    def coordinates(to):
        return (lax.div(to, grp), lax.rem(to, grp))

    def place(t):
        return coordinates(peer(t))

    def remote(src, dst, out_sem, in_sem, to):
        return pltpu.make_async_remote_copy(
            src_ref=src,
            dst_ref=dst,
            send_sem=out_sem,
            recv_sem=in_sem,
            device_id=coordinates(to),
            device_id_type=pl.DeviceIdType.MESH,
        )

    steps = [devices * k // 32 for k in GROUPS]

    def group_of(p):
        return sum((p >= edge) * 1 if isinstance(p, int) else (p >= edge).astype(jnp.int32) for edge in steps[1:-1])

    def feature(to, t, p):
        return remote(send.at[t], got.at[p], out_sems.at[1], group_sems.at[group_of(p)], to)

    def arrived(first, last):
        count = last - first - (first <= 1 < last)
        remote(
            send.at[pl.ds(0, count)],
            got.at[pl.ds(0, count)],
            out_sems.at[1],
            group_sems.at[group_of(first)],
            peer(1),
        ).wait_recv()

    pairs = (
        (front_hbm, front_ref),
        (req_hbm, req_ref),
        (req2_hbm, req2_ref),
        (table_hbm, table),
        (w1s_hbm, w1s_ref),
        (w1n_hbm, w1n_ref),
        (bias1_hbm, bias1_ref),
        (w2s_hbm, w2s_ref),
        (w2n_hbm, w2n_ref),
        (seed_hbm, seed_ref),
        (count1_hbm, count1_ref),
        (count2_hbm, count2_ref),
    )
    loads = [pltpu.make_async_copy(a, b, load_sems.at[i]) for i, (a, b) in enumerate(pairs)]
    for load in loads[:4]:
        load.start()
    barrier = pltpu.get_barrier_semaphore()
    for t in range(devices - 1, 0, -1):
        pl.semaphore_signal(
            barrier, inc=1, device_id=place(t), device_id_type=pl.DeviceIdType.MESH
        )
    for load in loads[4:]:
        load.start()
    loads[0].wait()
    prepare_list(front_ref, key1, unit1, first1, cap)
    loads[1].wait()
    loads[2].wait()
    for load in loads[9:]:
        load.wait()
    entry = seed_ref[...]
    owner, slot = entry >> (cap_two.bit_length() - 1), entry & (cap_two - 1)

    limit = jnp.zeros_like(entry)
    for o in range(devices):
        limit = jnp.where(owner == o, count2_ref[o], limit)
    live = slot < limit
    list_out[...] = jnp.where(live, entry, -1).astype(list_out.dtype)
    lists[0, 0] = list_out[...]
    early = devices * EARLY // 32

    def owner_at(p):
        return peer(step_of(p))

    count_slots(key1, unit1, first1, own, near, cap, owner_at, 0, early)
    loads[3].wait()
    step = 4 * LANES if rows.shape[0] % (4 * LANES) == 0 else LANES

    def transpose(i, carry):
        rows[tile(i, step), :] = table[:, tile(i, step)].T.astype(jnp.float32)
        return carry

    pieces = rows.shape[0] // step
    first_piece, second_piece = pieces // 8, pieces // 2
    lax.fori_loop(0, first_piece, transpose, 0)
    pl.semaphore_wait(barrier, devices - 1)

    couples = devices // 2

    def ask(t):
        return remote(req_ref.at[peer(t)], ids.at[t], out_sems.at[0], in_sems.at[0], peer(t))

    def ask_two(t):
        return remote(req2_ref.at[peer(t)], asked.at[t], out_sems.at[7], in_sems.at[4], peer(t))

    def give(i):
        return remote(list_out, lists.at[0, i], out_sems.at[2], in_sems.at[1], peer(2 * i))

    def hand_on():
        return remote(lists.at[0], lists.at[1], out_sems.at[3], in_sems.at[2], peer(1))

    for t in range(devices - 1, 0, -1):
        ask(t).start()
    own_ids = pltpu.make_async_copy(req_ref.at[me], ids.at[0], ids_sem)
    own_ids.start()
    for t in range(devices - 1, 0, -1):
        ask_two(t).start()
    asked[0] = req2_ref[me]
    lax.fori_loop(first_piece, second_piece, transpose, 0)
    for i in range(couples - 1, 0, -1):
        give(i).start()
    lax.fori_loop(second_piece, pieces, transpose, 0)
    own_ids.wait()
    rest = pl.ds(1, devices - 1)
    remote(req_ref.at[rest], ids.at[rest], out_sems.at[0], in_sems.at[0], peer(1)).wait()

    def pick(t, at):
        for j in range(cap):
            block[at, j : j + 1, :] = rows[pl.ds(ids[t, 0, j], 1), :]
        return block[at].T.astype(jnp.bfloat16)

    def pick_and_send(i, carry):
        to, before = peer(i), peer(i - 1)
        send[half + i] = pick(half + i, 0)
        send[i] = pick(i, 1)
        feature(lax.rem(before + half, devices), half + i - 1, 2 * i - 2).start()
        feature(before, i - 1, 2 * i - 1).start()
        return carry

    send[half] = pick(half, 0)
    send[half + 1] = pick(half + 1, 1)
    feature(peer(half), half, 0).start()
    send[1] = pick(1, 0)
    got[1] = pick(0, 1)
    lax.fori_loop(2, half, pick_and_send, 0)
    remote(req2_ref.at[rest], asked.at[rest], out_sems.at[7], in_sems.at[4], peer(1)).wait()
    onehot_slots(asked, onehot, cap_two, 0, 2)
    feature(peer(devices - 1), devices - 1, devices - 2).start()
    feature(peer(half - 1), half - 1, devices - 1).start()
    onehot_slots(asked, onehot, cap_two, 2, devices)
    for load in loads[4:9]:
        load.wait()
    width, hidden_width = w1s_ref.shape[0], w1.shape[0]
    wide = w1.shape[1] // 2
    classes, half_rows = w2s_ref.shape[0], w2.shape[0] // 2
    w1[...] = jnp.zeros_like(w1)
    w1[:, :width] = w1s_ref[...].T
    w1[:, wide : wide + width] = w1n_ref[...].T
    w2[...] = jnp.zeros_like(w2)
    w2[:classes] = w2s_ref[...]
    w2[half_rows : half_rows + classes] = w2n_ref[...]
    pair[...] = jnp.zeros_like(pair)
    bias1 = jnp.broadcast_to(bias1_ref[...], (8, hidden_width)).T[:, :1]

    remote(lists.at[0, pl.ds(0, couples - 1)], lists.at[0, pl.ds(1, couples - 1)], out_sems.at[2], in_sems.at[1], peer(1)).wait()
    hand_on().start()
    count_slots(key1, unit1, first1, own, near, cap, owner_at, early, devices)
    hand_on().wait()
    select_seeds(lists, key2, unit2, first2, select, me, cap_two, 0, devices)
    nodes = own.shape[0] * LANES
    chunk = 2 * LANES
    def lay(p, carry):
        slot = lax.broadcasted_iota(jnp.int32, got.shape[1:], 1)
        live = jnp.where(slot < count1_ref[owner_at(p)], got[p].astype(jnp.float32), 0.0)
        flat[p, :width, :] = live.astype(jnp.bfloat16)
        return carry

    def arrive(first, last):
        arrived(first, last)
        lax.fori_loop(first, last, lay, 0)

    arrive(0, steps[1])

    def side_by_side(parts):
        return jnp.concatenate(parts, axis=1)

    def picked(matrix, c, first, last):
        left = side_by_side([flat[p, :width, :] for p in range(first, last)])
        some = range(c * chunk // LANES, (c + 1) * chunk // LANES)
        return dot32(left, side_by_side([matrix[n, first * cap : last * cap, :] for n in some]))

    def add_up(first, last, fresh):
        for c in range(nodes // chunk):
            cols = slice(c * chunk, (c + 1) * chunk)
            for m, matrix in enumerate((own, near)):
                part = picked(matrix, c, first, last)
                acc[m, :, cols] = part if fresh else acc[m, :, cols] + part

    add_up(0, steps[1], True)
    for first, last in zip(steps[1:-2], steps[2:-1]):
        arrive(first, last)
        add_up(first, last, False)
    fan_two, fan_one = 1.0 / (front_ref.shape[0] - 1), 1.0 / (seed_ref.shape[0] - 1)
    arrive(steps[-2], steps[-1])
    scale = jnp.where(lax.broadcasted_iota(jnp.int32, (w2.shape[0], 1), 0) < half_rows, 1.0, fan_one)
    for c in range(nodes // chunk):
        cols = slice(c * chunk, (c + 1) * chunk)
        mine = acc[0, :, cols] + picked(own, c, steps[-2], steps[-1])
        summed = (acc[1, :, cols] + picked(near, c, steps[-2], steps[-1])) * fan_two
        for n in range(chunk // LANES):
            at, lanes = c * chunk // LANES + n, slice(n * LANES, (n + 1) * LANES)
            pair[at, :width, :] = mine[:, lanes].astype(jnp.bfloat16)
            pair[at, wide : wide + width, :] = summed[:, lanes].astype(jnp.bfloat16)
    hidden = []
    for c in range(nodes // chunk):
        some = range(c * chunk // LANES, (c + 1) * chunk // LANES)
        preact = dot32(w1[...], side_by_side([pair[n] for n in some])) + bias1
        hidden.append(jnp.maximum(preact, 0.0).astype(jnp.bfloat16))
    for c in range(nodes // chunk):
        last = (dot32(w2[...], hidden[c]) * scale).astype(jnp.bfloat16)
        for n in range(chunk // LANES):
            payload[c * chunk // LANES + n] = last[:, n * LANES : (n + 1) * LANES]
    across = term.shape[2] // LANES

    def choose(b):
        left = side_by_side([payload[n] for n in range(nodes // LANES)])
        for i in batches[b]:
            both = dot32(left, side_by_side([onehot[2 * i], onehot[2 * i + 1]])).astype(jnp.bfloat16)
            for c in range(2):
                cols = slice(c * cap_two, (c + 1) * cap_two)
                chosen[i, c, :, :cap_two] = both[:half_rows, cols]
                chosen[i, c, :, cap_two:] = both[half_rows:, cols]

    def terms(i):
        for c, out in ((1, term_out), (0, term)):
            at = (2 * i + c) * across
            out[i] = dot32(chosen[i, c], side_by_side([select[at + n] for n in range(across)]))

    moved, kept, direct = [], [], []
    for i in range(couples // 2, couples):
        (direct if i & 1 else moved if i & BRIDGE else kept).append(i)
    moved = [i ^ BRIDGE for i in kept]
    near_ones = list(range(1, couples // 2)) + [0]
    middle, some = len(near_ones) // 2, len(direct) // 2
    batches = (direct[:some], moved, direct[some:], kept, near_ones[:middle], near_ones[middle:])

    def prepare(b):
        for i in batches[b]:
            terms(i)
        for i in batches[b]:
            remote(
                term_out.at[i], term_in.at[i], out_sems.at[4], cross_sems.at[b], peer(1)
            ).start()

    def crossed(b):
        some = pl.ds(0, len(batches[b]))
        remote(
            term_out.at[some], term_in.at[some], out_sems.at[4], cross_sems.at[b], peer(1)
        ).wait_recv()

    def bridge(k):
        return remote(
            bridge_out.at[k], bridge_in.at[k], out_sems.at[6], bridge_sems.at[k], peer(2 * BRIDGE)
        )

    def away(i):
        return remote(send2.at[i], got2.at[i], out_sems.at[5], in_sems.at[3], peer(2 * i))

    def join(i):
        send2[i] = (term[i] + term_in[i]).astype(jnp.bfloat16)

    def join_and_send(b):
        for i in batches[b]:
            if i > 0:
                join(i)
        for i in batches[b]:
            if i > 0:
                away(i).start()

    choose(0)
    choose(1)
    prepare(0)
    choose(2)
    prepare(1)
    prepare(2)
    crossed(0)
    join_and_send(0)
    choose(3)
    choose(4)
    crossed(1)
    for k, i in enumerate(moved):
        bridge_out[k] = (term[i] + term_in[i]).astype(jnp.bfloat16)
    for k in range(len(moved)):
        bridge(k).start()
    prepare(3)
    prepare(4)
    choose(5)
    crossed(2)
    join_and_send(2)
    prepare(5)
    crossed(3)
    for i in kept:
        term[i] = term[i] + term_in[i]
    crossed(4)
    join_and_send(4)
    for k, i in enumerate(kept):
        bridge(k).wait_recv()
        send2[i] = (term[i] + bridge_in[k].astype(jnp.float32)).astype(jnp.bfloat16)
    for i in kept:
        away(i).start()
    crossed(5)
    join_and_send(5)
    total = term[0] + term_in[0]
    arriving = direct + kept + near_ones[:-1]
    for src, dst, k, sent in (
        (send, got, 1, devices - 1),
        (term_out, term_in, 4, couples),
        (bridge_out, bridge_in, 6, len(moved)),
        (send2, got2, 5, len(arriving)),
    ):
        whole = remote(src.at[pl.ds(0, sent)], dst.at[pl.ds(0, sent)], out_sems.at[k], in_sems.at[3], peer(1))
        if k == 5:
            whole.wait()
        else:
            whole.wait_send()
    for i in arriving:
        total = total + got2[i].astype(jnp.float32)
    out_ref[...] = total[:classes]


def mask_rows(received, counts, capacity):
    is_live = (jnp.arange(capacity, dtype=jnp.int32)[None, :] < counts[:, None]).reshape(-1)
    flat = received.reshape(-1, received.shape[-1])
    return jnp.where(is_live[:, None], flat, jnp.zeros((), flat.dtype))


def right_product(rows, weight):
    return lax.dot_general(
        rows, weight, (((1,), (1,)), ((), ())), preferred_element_type=jnp.float32
    )


def take_body(
    table_t,
    req_rows,
    count1,
    frontier_list,
    req2_rows,
    count2,
    seed_list,
    w1_self,
    w1_neigh,
    bias1,
    w2_self,
    w2_neigh,
    bias2,
):
    feat_width = table_t.shape[0]
    capacity = req_rows.shape[1]
    table_rows = table_t.T
    picked_rows = jnp.take(
        table_rows,
        lax.all_to_all(req_rows, AXES, split_axis=0, concat_axis=0, tiled=True),
        axis=0,
    )
    received = lax.all_to_all(
        picked_rows, AXES, split_axis=0, concat_axis=0, tiled=True
    )
    flat = mask_rows(received, count1, capacity)
    fanout_two = frontier_list.shape[0] - 1
    front_nodes = frontier_list.shape[1]
    picked = jnp.take(flat, frontier_list.reshape(-1), axis=0).reshape(
        fanout_two + 1, front_nodes, feat_width
    )
    summed = (jnp.sum(picked[1:].astype(jnp.float32), axis=0) / fanout_two).astype(jnp.bfloat16)
    preact = right_product(picked[0], w1_self) + right_product(summed, w1_neigh) + bias1[None, :]
    hidden_rows = jax.nn.relu(preact).astype(jnp.bfloat16)
    cap_two = req2_rows.shape[1]
    payload = jnp.concatenate(
        [right_product(hidden_rows, w2_self), right_product(hidden_rows, w2_neigh)], axis=1
    )
    chosen = jnp.take(
        payload,
        lax.all_to_all(req2_rows, AXES, split_axis=0, concat_axis=0, tiled=True),
        axis=0,
    )
    got_back = lax.all_to_all(chosen, AXES, split_axis=0, concat_axis=0, tiled=True)
    flat_two = mask_rows(got_back, count2, cap_two)
    fanout_one = seed_list.shape[0] - 1
    seed_nodes = seed_list.shape[1]
    picked_two = jnp.take(flat_two, seed_list.reshape(-1), axis=0).reshape(
        fanout_one + 1, seed_nodes, flat_two.shape[1]
    )
    classes = w2_self.shape[0]
    near = jnp.sum(picked_two[1:, :, classes:], axis=0) / fanout_one
    logits = (picked_two[0, :, :classes] + near).T + bias2[:, None]
    return logits


def body(
    table_t,
    req_rows,
    count1,
    frontier_list,
    req2_rows,
    count2,
    seed_list,
    w1_self,
    w1_neigh,
    bias1,
    w2_self,
    w2_neigh,
    bias2,
):
    devices, cap = req_rows.shape
    cap_two = req2_rows.shape[1]
    nodes = frontier_list.shape[1]
    small = devices * max(cap, cap_two) * nodes <= MATRIX_LIMIT
    even = devices >= 32 and devices & (devices - 1) == 0
    plain = cap == cap_two == LANES and nodes % (2 * LANES) == 0
    few = max(frontier_list.shape[0], seed_list.shape[0]) <= 2**FIELD_BITS
    if not (small and even and plain and few):
        return take_body(
            table_t,
            req_rows,
            count1,
            frontier_list,
            req2_rows,
            count2,
            seed_list,
            w1_self,
            w1_neigh,
            bias1,
            w2_self,
            w2_neigh,
            bias2,
        )
    width, table_rows = table_t.shape
    entries, entries_two = frontier_list.shape[0], seed_list.shape[0]
    seeds = seed_list.shape[1]
    hidden_width, classes = w1_self.shape[0], w2_self.shape[0]
    rows_two = 2 * (-(-classes // 16) * 16)
    bf16, f32, i32 = jnp.bfloat16, jnp.float32, jnp.int32
    logits = pl.pallas_call(
        functools.partial(whole_kernel, lax.axis_size(AXES[1]), rows_two),
        in_specs=[pl.BlockSpec(memory_space=pl.ANY)] * 12,
        out_specs=pl.BlockSpec(memory_space=pltpu.VMEM),
        out_shape=jax.ShapeDtypeStruct((classes, seeds), f32),
        scratch_shapes=[
            pltpu.VMEM((width, table_rows), bf16),
            pltpu.VMEM((devices, 1, cap), i32),
            pltpu.VMEM((devices, 1, cap_two), i32),
            pltpu.SMEM((devices,), i32),
            pltpu.SMEM((devices,), i32),
            pltpu.VMEM((entries, nodes), i32),
            pltpu.VMEM((entries_two, seeds), i32),
            pltpu.VMEM((width, hidden_width), bf16),
            pltpu.VMEM((width, hidden_width), bf16),
            pltpu.VMEM((1, hidden_width), f32),
            pltpu.VMEM((classes, hidden_width), bf16),
            pltpu.VMEM((classes, hidden_width), bf16),
            pltpu.VMEM((entries, nodes), i32),
            pltpu.VMEM((entries, nodes), i32),
            pltpu.VMEM((1, nodes), f32),
            pltpu.VMEM((entries_two, seeds), i32),
            pltpu.VMEM((entries_two, seeds), i32),
            pltpu.VMEM((1, seeds), f32),
            pltpu.VMEM((devices, 1, cap_two), i32),
            pltpu.SMEM((devices, 1, cap), i32),
            pltpu.VMEM((table_rows, width), f32),
            pltpu.VMEM((2, cap, width), f32),
            pltpu.VMEM((devices, width, cap), bf16),
            pltpu.VMEM((devices, width, cap), bf16),
            pltpu.VMEM((entries_two, seeds), jnp.int16),
            pltpu.VMEM((2, devices // 2, entries_two, seeds), jnp.int16),
            pltpu.VMEM((2, width, nodes), f32),
            pltpu.VMEM((devices // 2, rows_two // 2, seeds), f32),
            pltpu.VMEM((devices // 2, rows_two // 2, seeds), f32),
            pltpu.VMEM((devices // 2, rows_two // 2, seeds), f32),
            pltpu.VMEM((devices // 2, rows_two // 2, seeds), bf16),
            pltpu.VMEM((devices // 2, rows_two // 2, seeds), bf16),
            pltpu.VMEM((devices // 16, rows_two // 2, seeds), bf16),
            pltpu.VMEM((devices // 16, rows_two // 2, seeds), bf16),
            pltpu.SemaphoreType.DMA((12,)),
            pltpu.SemaphoreType.DMA,
            pltpu.SemaphoreType.DMA((8,)),
            pltpu.SemaphoreType.DMA((5,)),
            pltpu.SemaphoreType.DMA((len(GROUPS) - 1,)),
            pltpu.SemaphoreType.DMA((6,)),
            pltpu.SemaphoreType.DMA((devices // 16,)),
        ],
        compiler_params=pltpu.CompilerParams(
            vmem_limit_bytes=63 * MIB, collective_id=0, has_side_effects=True
        ),
    )(
        table_t,
        req_rows[:, None, :],
        req2_rows[:, None, :],
        count1,
        count2,
        frontier_list,
        seed_list,
        w1_self.T,
        w1_neigh.T,
        bias1[None, :],
        w2_self,
        w2_neigh,
    )
    return logits + bias2[:, None]


def solution(mesh):
    in_specs = (
        P(None, AXES),
        P(AXES, None),
        P(AXES),
        P(None, AXES),
        P(AXES, None),
        P(AXES),
        P(None, AXES),
        P(),
        P(),
        P(),
        P(),
        P(),
        P(),
    )
    return jax.shard_map(
        body, mesh=mesh, in_specs=in_specs, out_specs=P(None, AXES), check_vma=False
    )
```

```python
import functools

import jax
import jax.numpy as jnp
from jax import lax
from jax.experimental import pallas as pl
from jax.experimental.pallas import tpu as pltpu
from jax.sharding import PartitionSpec as P

AXES = ("shard", "grp")
LANES = 128
MIB = 1024 * 1024
MATRIX_LIMIT = 4 * MIB
EARLY = 2
GROUPS = (0, 16, 24, 30, 32)
BRIDGE = 2


FIELDS = 8
FIELD_BITS = 4


def tile(i, size=LANES):
    return pl.ds(pl.multiple_of(i * size, size), size)


def dot32(a, b):
    return jnp.dot(a, b, preferred_element_type=jnp.float32)


def tile_names(span):
    first = lax.broadcasted_iota(jnp.int32, (16, LANES), 0).astype(jnp.float32)
    return [(first + float(16 * b)).astype(jnp.bfloat16) for b in range(span // 16)]


def hits(row, names):
    few = jnp.broadcast_to(row, (16, row.shape[1])).astype(jnp.bfloat16)
    one, zero = jnp.ones((), jnp.bfloat16), jnp.zeros((), jnp.bfloat16)
    return [jnp.where(few == name, one, zero) for name in names]


def prepare_list(list_ref, key_ref, unit_ref, first_ref, cap):
    words = cap // FIELDS
    entry = list_ref[...]
    owner, slot = entry >> (cap.bit_length() - 1), entry & (cap - 1)
    key_ref[...] = owner * words + (slot & (words - 1))
    unit_ref[...] = jnp.ones((), jnp.int32) << (FIELD_BITS * (slot >> (words.bit_length() - 1)))
    first_ref[...] = entry[0:1].astype(jnp.float32)


def count_tile(key_ref, unit_ref, first, name, names, own_ref, near_ref, own_at, near_at, cols, to):
    words = name.shape[0]
    total = jnp.zeros(name.shape, jnp.int32)
    for k in range(1, key_ref.shape[0]):
        total = total + jnp.where(key_ref[k : k + 1, cols] == name, unit_ref[k : k + 1, cols], 0)
    for b in range(FIELDS):
        field = (total >> (FIELD_BITS * b)) & (2**FIELD_BITS - 1)
        near_ref[to, pl.ds(pl.multiple_of(near_at + b * words, words), words), :] = field.astype(
            jnp.float32
        ).astype(jnp.bfloat16)
    for b, part in enumerate(hits(first, names)):
        own_ref[to, pl.ds(pl.multiple_of(own_at + b * 16, 16), 16), :] = part


def count_slots(key_ref, unit_ref, first_ref, own_ref, near_ref, cap, owner_of, first, last):
    across = key_ref.shape[1] // LANES
    some = 4 if across % 4 == 0 else 1
    words = cap // FIELDS
    names = tile_names(cap)
    low = lax.broadcasted_iota(jnp.int32, (words, LANES), 0)

    def one(i, carry):
        at, base = lax.div(i, across // some), lax.rem(i, across // some) * some
        owner = owner_of(at)
        name, start = low + owner * words, (owner * cap).astype(jnp.float32)
        for c in range(some):
            cols = tile(base + c)
            own = first_ref[0:1, cols] - start
            count_tile(
                key_ref, unit_ref, own, name, names, own_ref, near_ref, at * cap, at * cap, cols, base + c
            )
        return carry

    lax.fori_loop(first * (across // some), last * (across // some), one, 0)


def select_seeds(lists_ref, key_ref, unit_ref, first_ref, out_ref, me, cap, first, last):
    devices, _, seeds = lists_ref.shape
    depth = devices // 8

    def step_at(at):
        core, y = lax.div(at, 4 * depth), lax.rem(lax.div(at, 2 * depth), 2)
        return core + 2 * y + 4 * lax.rem(lax.div(at, depth), 2) + 8 * lax.rem(at, depth)

    words = cap // FIELDS
    names = tile_names(cap)
    low = lax.broadcasted_iota(jnp.int32, (words, LANES), 0)

    def one(at, carry):
        local = lists_ref[at].astype(jnp.int32) - me * cap
        field = local >> (words.bit_length() - 1)
        here = jnp.logical_and(field >= 0, field < FIELDS)
        key_ref[...] = local & (words - 1)
        unit_ref[...] = jnp.where(here, jnp.ones((), jnp.int32) << (FIELD_BITS * (field & (FIELDS - 1))), 0)
        first_ref[...] = local[0:1].astype(jnp.float32)
        for c in range(seeds // LANES):
            cols = slice(c * LANES, (c + 1) * LANES)
            to = step_at(at) * (seeds // LANES) + c
            count_tile(
                key_ref, unit_ref, first_ref[0:1, cols], low, names, out_ref, out_ref, 0, cap, cols, to
            )
        return carry

    lax.fori_loop(first, last, one, 0)


def onehot_slots(asked_ref, out_ref, cap, first, last):
    nodes = out_ref.shape[1]
    names = tile_names(LANES)

    def one(t, carry):
        wanted = asked_ref[t].astype(jnp.float32)
        for b in range(nodes // LANES):
            for c, part in enumerate(hits(wanted - float(b * LANES), names)):
                out_ref[t, b * LANES + 16 * c : b * LANES + 16 * c + 16, :] = part
        return carry

    lax.fori_loop(first, last, one, 0)


def whole_kernel(grp, rows_two, *refs):
    req_hbm, req2_hbm, front_hbm, seed_hbm, w1s_hbm, w2s_hbm = (refs[k] for k in (1, 2, 5, 6, 7, 10))
    devices, cap, cap_two = req_hbm.shape[0], req_hbm.shape[2], req2_hbm.shape[2]
    nodes, seeds = front_hbm.shape[1], seed_hbm.shape[1]
    width, hidden_width = w1s_hbm.shape
    wide = -(-width // LANES) * LANES
    bf16 = jnp.bfloat16
    pl.run_scoped(
        functools.partial(inner_kernel, grp, *refs),
        pltpu.VMEM((hidden_width, 2 * wide), bf16),
        pltpu.VMEM((rows_two, hidden_width), bf16),
        pltpu.VMEM((nodes // LANES, devices * cap, LANES), bf16),
        pltpu.VMEM((nodes // LANES, devices * cap, LANES), bf16),
        pltpu.VMEM((devices, nodes, LANES), bf16),
        pltpu.VMEM((devices * seeds // LANES, 2 * cap_two, LANES), bf16),
        pltpu.VMEM((devices, -(-width // 16) * 16, cap), bf16),
        pltpu.VMEM((nodes // LANES, 2 * wide, LANES), bf16),
        pltpu.VMEM((nodes // LANES, rows_two, LANES), bf16),
        pltpu.VMEM((devices // 2, 2, rows_two // 2, 2 * cap_two), bf16),
    )


def inner_kernel(
    grp,
    table_hbm,
    req_hbm,
    req2_hbm,
    count1_hbm,
    count2_hbm,
    front_hbm,
    seed_hbm,
    w1s_hbm,
    w1n_hbm,
    bias1_hbm,
    w2s_hbm,
    w2n_hbm,
    out_ref,
    table,
    req_ref,
    req2_ref,
    count1_ref,
    count2_ref,
    front_ref,
    seed_ref,
    w1s_ref,
    w1n_ref,
    bias1_ref,
    w2s_ref,
    w2n_ref,
    key1,
    unit1,
    first1,
    key2,
    unit2,
    first2,
    asked,
    ids,
    rows,
    block,
    send,
    got,
    send_rest,
    got_rest,
    lists,
    acc,
    term_out,
    term_in,
    term,
    send2,
    got2,
    bridge_out,
    bridge_in,
    load_sems,
    ids_sem,
    out_sems,
    in_sems,
    group_sems,
    cross_sems,
    bridge_sems,
    ask_sems,
    list_sems,
    w1,
    w2,
    own,
    near,
    onehot,
    select,
    flat,
    pair,
    payload,
    chosen,
):
    devices, _, cap = req_ref.shape
    cap_two = req2_ref.shape[2]
    me = lax.axis_index(AXES[0]) * grp + lax.axis_index(AXES[1])
    half = devices // 2
    bits = devices.bit_length() - 1

    def peer(t):
        total = 0
        for i in range(bits):
            mine = lax.rem(lax.div(me, 2**i), 2)
            if isinstance(t, int):
                bit = 1 - mine if (t >> i) & 1 else mine
            else:
                other = lax.rem(lax.div(t, 2**i), 2)
                bit = mine + other - 2 * mine * other
            total = total + bit * 2**i
        return total

    def step_of(p):
        return half * (1 - lax.rem(p, 2)) + lax.div(p, 2)

    def coordinates(to):
        return (lax.div(to, grp), lax.rem(to, grp))

    def place(t):
        return coordinates(peer(t))

    def remote(src, dst, out_sem, in_sem, to):
        return pltpu.make_async_remote_copy(
            src_ref=src,
            dst_ref=dst,
            send_sem=out_sem,
            recv_sem=in_sem,
            device_id=coordinates(to),
            device_id_type=pl.DeviceIdType.MESH,
        )

    steps = [devices * k // 32 for k in GROUPS]

    def group_of(p):
        return sum((p >= edge) * 1 if isinstance(p, int) else (p >= edge).astype(jnp.int32) for edge in steps[1:-1])

    def feature(to, t, p):
        group = group_of(p)
        remote(send.at[t], got.at[p], out_sems.at[1], group_sems.at[0, group], to).start()
        remote(
            send_rest.at[t], got_rest.at[p], out_sems.at[8], group_sems.at[1, group], to
        ).start()

    def arrived(first, last):
        count = last - first - (first <= 1 < last)
        group = group_of(first)
        some = pl.ds(0, count)
        remote(
            send.at[some], got.at[some], out_sems.at[1], group_sems.at[0, group], peer(1)
        ).wait_recv()
        remote(
            send_rest.at[some], got_rest.at[some], out_sems.at[8], group_sems.at[1, group], peer(1)
        ).wait_recv()

    pairs = (
        (front_hbm, front_ref),
        (req_hbm, req_ref),
        (req2_hbm, req2_ref),
        (table_hbm, table),
        (w1s_hbm, w1s_ref),
        (w1n_hbm, w1n_ref),
        (bias1_hbm, bias1_ref),
        (w2s_hbm, w2s_ref),
        (w2n_hbm, w2n_ref),
        (seed_hbm, seed_ref),
        (count1_hbm, count1_ref),
        (count2_hbm, count2_ref),
    )
    loads = [pltpu.make_async_copy(a, b, load_sems.at[i]) for i, (a, b) in enumerate(pairs)]
    for load in loads[:4]:
        load.start()
    barrier = pltpu.get_barrier_semaphore()
    for t in range(devices - 1, 0, -1):
        pl.semaphore_signal(
            barrier, inc=1, device_id=place(t), device_id_type=pl.DeviceIdType.MESH
        )
    for load in loads[4:]:
        load.start()
    loads[0].wait()
    prepare_list(front_ref, key1, unit1, first1, cap)
    loads[1].wait()
    loads[2].wait()
    for load in loads[9:]:
        load.wait()
    entry = seed_ref[...]
    owner, slot = entry >> (cap_two.bit_length() - 1), entry & (cap_two - 1)

    limit = jnp.zeros_like(entry)
    for o in range(devices):
        limit = jnp.where(owner == o, count2_ref[o], limit)
    live = slot < limit
    lists[0] = jnp.where(live, entry, -1).astype(lists.dtype)
    early = devices * EARLY // 32

    def owner_at(p):
        return peer(step_of(p))

    count_slots(key1, unit1, first1, own, near, cap, owner_at, 0, early)
    loads[3].wait()
    step = 4 * LANES if rows.shape[0] % (4 * LANES) == 0 else LANES

    def transpose(i, carry):
        rows[tile(i, step), :] = table[:, tile(i, step)].T.astype(jnp.float32)
        return carry

    pieces = rows.shape[0] // step
    first_piece, second_piece = pieces // 8, pieces // 2
    lax.fori_loop(0, first_piece, transpose, 0)
    pl.semaphore_wait(barrier, devices - 1)

    couples = devices // 2

    def ask(t):
        quarter = t % half // (half // 4)
        return remote(req_ref.at[peer(t)], ids.at[t], out_sems.at[0], ask_sems.at[quarter], peer(t))

    def ask_two(t):
        return remote(req2_ref.at[peer(t)], asked.at[t], out_sems.at[7], in_sems.at[4], peer(t))

    def hand_on(k):
        depth = devices // 8
        if k == 0:
            return [
                remote(lists.at[0], lists.at[j], list_sems.at[0, 0], list_sems.at[1, 0], peer(8 * j))
                for j in range(1, depth)
            ]
        count = depth << (k - 1)
        return [
            remote(
                lists.at[pl.ds(0, count)],
                lists.at[pl.ds(count, count)],
                list_sems.at[0, k],
                list_sems.at[1, k],
                peer(8 >> k),
            )
        ]

    def take(k):
        if k == 0:
            some = pl.ds(0, devices // 8 - 1)
            remote(
                lists.at[some], lists.at[some], list_sems.at[0, 0], list_sems.at[1, 0], peer(1)
            ).wait()
        else:
            hand_on(k)[0].wait()

    for t in range(devices - 1, 0, -1):
        ask(t).start()
    own_ids = pltpu.make_async_copy(req_ref.at[me], ids.at[0], ids_sem)
    own_ids.start()
    for t in range(devices - 1, 0, -1):
        ask_two(t).start()
    asked[0] = req2_ref[me]
    for one in hand_on(0):
        one.start()
    lax.fori_loop(first_piece, second_piece, transpose, 0)
    lax.fori_loop(second_piece, pieces, transpose, 0)
    own_ids.wait()
    rest = pl.ds(1, devices - 1)

    def asked_for(count, k):
        some = pl.ds(0, count)
        return remote(req_ref.at[some], ids.at[some], out_sems.at[0], ask_sems.at[k], peer(1))

    asked_for(half // 2 - 1, 0).wait_recv()

    main = send.shape[1]

    def pick(t, at):
        for j in range(cap):
            block[at, j : j + 1, :] = rows[pl.ds(ids[t, 0, j], 1), :]
        columns = block[at].T.astype(jnp.bfloat16)
        return columns[:main], columns[main:]

    def put(to, rest, at, columns):
        to[at], rest[at] = columns

    def pick_and_send(i, carry):
        to, before = peer(i), peer(i - 1)
        put(send, send_rest, half + i, pick(half + i, 0))
        put(send, send_rest, i, pick(i, 1))
        feature(lax.rem(before + half, devices), half + i - 1, 2 * i - 2)
        feature(before, i - 1, 2 * i - 1)
        return carry

    put(send, send_rest, half, pick(half, 0))
    put(send, send_rest, half + 1, pick(half + 1, 1))
    feature(peer(half), half, 0)
    put(send, send_rest, 1, pick(1, 0))
    put(got, got_rest, 1, pick(0, 1))
    lax.fori_loop(2, half // 4, pick_and_send, 0)
    take(0)
    hand_on(1)[0].start()
    for k in range(1, 4):
        asked_for(half // 2, k).wait_recv()
        lax.fori_loop(k * half // 4, (k + 1) * half // 4, pick_and_send, 0)
    asked_for(devices - 1, 0).wait_send()
    remote(req2_ref.at[rest], asked.at[rest], out_sems.at[7], in_sems.at[4], peer(1)).wait()
    onehot_slots(asked, onehot, cap_two, 0, 2)
    feature(peer(devices - 1), devices - 1, devices - 2)
    feature(peer(half - 1), half - 1, devices - 1)
    onehot_slots(asked, onehot, cap_two, 2, devices)
    for load in loads[4:9]:
        load.wait()
    width, hidden_width = w1s_ref.shape[0], w1.shape[0]
    wide = w1.shape[1] // 2
    classes, half_rows = w2s_ref.shape[0], w2.shape[0] // 2
    w1[...] = jnp.zeros_like(w1)
    w1[:, :width] = w1s_ref[...].T
    w1[:, wide : wide + width] = w1n_ref[...].T
    w2[...] = jnp.zeros_like(w2)
    w2[:classes] = w2s_ref[...]
    w2[half_rows : half_rows + classes] = w2n_ref[...]
    pair[...] = jnp.zeros_like(pair)
    bias1 = jnp.broadcast_to(bias1_ref[...], (8, hidden_width)).T[:, :1]

    take(1)
    hand_on(2)[0].start()
    count_slots(key1, unit1, first1, own, near, cap, owner_at, early, devices * 5 // 8)
    take(2)
    hand_on(3)[0].start()
    count_slots(key1, unit1, first1, own, near, cap, owner_at, devices * 5 // 8, devices)
    take(3)
    select_seeds(lists, key2, unit2, first2, select, me, cap_two, 0, devices)
    nodes = own.shape[0] * LANES
    chunk = 2 * LANES
    def lay(p, carry):
        count = count1_ref[owner_at(p)]
        for part, at, rows_here in ((got, 0, main), (got_rest, main, got_rest.shape[1])):
            slot = lax.broadcasted_iota(jnp.int32, part.shape[1:], 1)
            live = jnp.where(slot < count, part[p].astype(jnp.float32), 0.0)
            flat[p, at : at + rows_here, :] = live.astype(jnp.bfloat16)
        return carry

    def arrive(first, last):
        arrived(first, last)
        lax.fori_loop(first, last, lay, 0)

    arrive(0, steps[1])

    def side_by_side(parts):
        return jnp.concatenate(parts, axis=1)

    def picked(matrix, c, first, last):
        left = side_by_side([flat[p, :width, :] for p in range(first, last)])
        some = range(c * chunk // LANES, (c + 1) * chunk // LANES)
        return dot32(left, side_by_side([matrix[n, first * cap : last * cap, :] for n in some]))

    def add_up(first, last, fresh):
        for c in range(nodes // chunk):
            cols = slice(c * chunk, (c + 1) * chunk)
            for m, matrix in enumerate((own, near)):
                part = picked(matrix, c, first, last)
                acc[m, :, cols] = part if fresh else acc[m, :, cols] + part

    add_up(0, steps[1], True)
    for first, last in zip(steps[1:-2], steps[2:-1]):
        arrive(first, last)
        add_up(first, last, False)
    fan_two, fan_one = 1.0 / (front_ref.shape[0] - 1), 1.0 / (seed_ref.shape[0] - 1)
    arrive(steps[-2], steps[-1])
    scale = jnp.where(lax.broadcasted_iota(jnp.int32, (w2.shape[0], 1), 0) < half_rows, 1.0, fan_one)
    for c in range(nodes // chunk):
        cols = slice(c * chunk, (c + 1) * chunk)
        mine = acc[0, :, cols] + picked(own, c, steps[-2], steps[-1])
        summed = (acc[1, :, cols] + picked(near, c, steps[-2], steps[-1])) * fan_two
        for n in range(chunk // LANES):
            at, lanes = c * chunk // LANES + n, slice(n * LANES, (n + 1) * LANES)
            pair[at, :width, :] = mine[:, lanes].astype(jnp.bfloat16)
            pair[at, wide : wide + width, :] = summed[:, lanes].astype(jnp.bfloat16)
    hidden = []
    for c in range(nodes // chunk):
        some = range(c * chunk // LANES, (c + 1) * chunk // LANES)
        preact = dot32(w1[...], side_by_side([pair[n] for n in some])) + bias1
        hidden.append(jnp.maximum(preact, 0.0).astype(jnp.bfloat16))
    for c in range(nodes // chunk):
        last = (dot32(w2[...], hidden[c]) * scale).astype(jnp.bfloat16)
        for n in range(chunk // LANES):
            payload[c * chunk // LANES + n] = last[:, n * LANES : (n + 1) * LANES]
    across = term.shape[2] // LANES

    def choose(b):
        left = side_by_side([payload[n] for n in range(nodes // LANES)])
        for i in batches[b]:
            both = dot32(left, side_by_side([onehot[2 * i], onehot[2 * i + 1]])).astype(jnp.bfloat16)
            for c in range(2):
                cols = slice(c * cap_two, (c + 1) * cap_two)
                chosen[i, c, :, :cap_two] = both[:half_rows, cols]
                chosen[i, c, :, cap_two:] = both[half_rows:, cols]

    def terms(i):
        for c, out in ((1, term_out), (0, term)):
            at = (2 * i + c) * across
            out[i] = dot32(chosen[i, c], side_by_side([select[at + n] for n in range(across)]))

    moved, kept, direct = [], [], []
    for i in range(couples // 2, couples):
        (direct if i & 1 else moved if i & BRIDGE else kept).append(i)
    moved = [i ^ BRIDGE for i in kept]
    near_ones = [*range(couples // 4, couples // 2), *range(1, couples // 4), 0]
    middle, some = len(near_ones) // 2, len(direct) // 2
    batches = (moved, direct[:some], direct[some:], kept, near_ones[:middle], near_ones[middle:])

    def prepare(b):
        for i in batches[b]:
            terms(i)
        for i in batches[b]:
            remote(
                term_out.at[i], term_in.at[i], out_sems.at[4], cross_sems.at[b], peer(1)
            ).start()

    def crossed(b):
        some = pl.ds(0, len(batches[b]))
        remote(
            term_out.at[some], term_in.at[some], out_sems.at[4], cross_sems.at[b], peer(1)
        ).wait_recv()

    def bridge(k):
        return remote(
            bridge_out.at[k], bridge_in.at[k], out_sems.at[6], bridge_sems.at[k], peer(2 * BRIDGE)
        )

    def away(i):
        return remote(send2.at[i], got2.at[i], out_sems.at[5], in_sems.at[3], peer(2 * i))

    def join(i):
        send2[i] = (term[i] + term_in[i]).astype(jnp.bfloat16)

    def join_and_send(b):
        for i in batches[b]:
            if i > 0:
                join(i)
        for i in batches[b]:
            if i > 0:
                away(i).start()

    choose(0)
    choose(1)
    prepare(0)
    choose(2)
    prepare(1)
    crossed(0)
    for k, i in enumerate(moved):
        bridge_out[k] = (term[i] + term_in[i]).astype(jnp.bfloat16)
    for k in range(len(moved)):
        bridge(k).start()
    choose(4)
    prepare(2)
    crossed(1)
    join_and_send(1)
    choose(3)
    prepare(4)
    choose(5)
    prepare(3)
    crossed(2)
    join_and_send(2)
    prepare(5)
    crossed(4)
    join_and_send(4)
    crossed(3)
    for i in kept:
        term[i] = term[i] + term_in[i]
    crossed(5)
    join_and_send(5)
    for k, i in enumerate(kept):
        bridge(k).wait_recv()
        send2[i] = (term[i] + bridge_in[k].astype(jnp.float32)).astype(jnp.bfloat16)
    for i in kept:
        away(i).start()
    total = term[0] + term_in[0]
    arriving = direct + kept + near_ones[:-1]
    for src, dst, k, sent in (
        (send, got, 1, devices - 1),
        (send_rest, got_rest, 8, devices - 1),
        (term_out, term_in, 4, couples),
        (bridge_out, bridge_in, 6, len(moved)),
        (send2, got2, 5, len(arriving)),
    ):
        whole = remote(src.at[pl.ds(0, sent)], dst.at[pl.ds(0, sent)], out_sems.at[k], in_sems.at[3], peer(1))
        if k == 5:
            whole.wait()
        else:
            whole.wait_send()
    for i in arriving:
        total = total + got2[i].astype(jnp.float32)
    out_ref[...] = total[:classes]


def mask_rows(received, counts, capacity):
    is_live = (jnp.arange(capacity, dtype=jnp.int32)[None, :] < counts[:, None]).reshape(-1)
    flat = received.reshape(-1, received.shape[-1])
    return jnp.where(is_live[:, None], flat, jnp.zeros((), flat.dtype))


def right_product(rows, weight):
    return lax.dot_general(
        rows, weight, (((1,), (1,)), ((), ())), preferred_element_type=jnp.float32
    )


def take_body(
    table_t,
    req_rows,
    count1,
    frontier_list,
    req2_rows,
    count2,
    seed_list,
    w1_self,
    w1_neigh,
    bias1,
    w2_self,
    w2_neigh,
    bias2,
):
    feat_width = table_t.shape[0]
    capacity = req_rows.shape[1]
    table_rows = table_t.T
    picked_rows = jnp.take(
        table_rows,
        lax.all_to_all(req_rows, AXES, split_axis=0, concat_axis=0, tiled=True),
        axis=0,
    )
    received = lax.all_to_all(
        picked_rows, AXES, split_axis=0, concat_axis=0, tiled=True
    )
    flat = mask_rows(received, count1, capacity)
    fanout_two = frontier_list.shape[0] - 1
    front_nodes = frontier_list.shape[1]
    picked = jnp.take(flat, frontier_list.reshape(-1), axis=0).reshape(
        fanout_two + 1, front_nodes, feat_width
    )
    summed = (jnp.sum(picked[1:].astype(jnp.float32), axis=0) / fanout_two).astype(jnp.bfloat16)
    preact = right_product(picked[0], w1_self) + right_product(summed, w1_neigh) + bias1[None, :]
    hidden_rows = jax.nn.relu(preact).astype(jnp.bfloat16)
    cap_two = req2_rows.shape[1]
    payload = jnp.concatenate(
        [right_product(hidden_rows, w2_self), right_product(hidden_rows, w2_neigh)], axis=1
    )
    chosen = jnp.take(
        payload,
        lax.all_to_all(req2_rows, AXES, split_axis=0, concat_axis=0, tiled=True),
        axis=0,
    )
    got_back = lax.all_to_all(chosen, AXES, split_axis=0, concat_axis=0, tiled=True)
    flat_two = mask_rows(got_back, count2, cap_two)
    fanout_one = seed_list.shape[0] - 1
    seed_nodes = seed_list.shape[1]
    picked_two = jnp.take(flat_two, seed_list.reshape(-1), axis=0).reshape(
        fanout_one + 1, seed_nodes, flat_two.shape[1]
    )
    classes = w2_self.shape[0]
    near = jnp.sum(picked_two[1:, :, classes:], axis=0) / fanout_one
    logits = (picked_two[0, :, :classes] + near).T + bias2[:, None]
    return logits


def body(
    table_t,
    req_rows,
    count1,
    frontier_list,
    req2_rows,
    count2,
    seed_list,
    w1_self,
    w1_neigh,
    bias1,
    w2_self,
    w2_neigh,
    bias2,
):
    devices, cap = req_rows.shape
    cap_two = req2_rows.shape[1]
    nodes = frontier_list.shape[1]
    small = devices * max(cap, cap_two) * nodes <= MATRIX_LIMIT
    even = devices >= 32 and devices & (devices - 1) == 0
    plain = cap == cap_two == LANES and nodes % (2 * LANES) == 0
    plain = plain and table_t.shape[0] > 16
    few = max(frontier_list.shape[0], seed_list.shape[0]) <= 2**FIELD_BITS
    if not (small and even and plain and few):
        return take_body(
            table_t,
            req_rows,
            count1,
            frontier_list,
            req2_rows,
            count2,
            seed_list,
            w1_self,
            w1_neigh,
            bias1,
            w2_self,
            w2_neigh,
            bias2,
        )
    width, table_rows = table_t.shape
    entries, entries_two = frontier_list.shape[0], seed_list.shape[0]
    seeds = seed_list.shape[1]
    hidden_width, classes = w1_self.shape[0], w2_self.shape[0]
    rows_two = 2 * (-(-classes // 16) * 16)
    bf16, f32, i32 = jnp.bfloat16, jnp.float32, jnp.int32
    main = (width - 1) // 16 * 16
    logits = pl.pallas_call(
        functools.partial(whole_kernel, lax.axis_size(AXES[1]), rows_two),
        in_specs=[pl.BlockSpec(memory_space=pl.ANY)] * 12,
        out_specs=pl.BlockSpec(memory_space=pltpu.VMEM),
        out_shape=pltpu.VMEM((classes, seeds), f32),
        scratch_shapes=[
            pltpu.VMEM((width, table_rows), bf16),
            pltpu.VMEM((devices, 1, cap), i32),
            pltpu.VMEM((devices, 1, cap_two), i32),
            pltpu.SMEM((devices,), i32),
            pltpu.SMEM((devices,), i32),
            pltpu.VMEM((entries, nodes), i32),
            pltpu.VMEM((entries_two, seeds), i32),
            pltpu.VMEM((width, hidden_width), bf16),
            pltpu.VMEM((width, hidden_width), bf16),
            pltpu.VMEM((1, hidden_width), f32),
            pltpu.VMEM((classes, hidden_width), bf16),
            pltpu.VMEM((classes, hidden_width), bf16),
            pltpu.VMEM((entries, nodes), i32),
            pltpu.VMEM((entries, nodes), i32),
            pltpu.VMEM((1, nodes), f32),
            pltpu.VMEM((entries_two, seeds), i32),
            pltpu.VMEM((entries_two, seeds), i32),
            pltpu.VMEM((1, seeds), f32),
            pltpu.VMEM((devices, 1, cap_two), i32),
            pltpu.SMEM((devices, 1, cap), i32),
            pltpu.VMEM((table_rows, width), f32),
            pltpu.VMEM((2, cap, width), f32),
            pltpu.VMEM((devices, main, cap), bf16),
            pltpu.VMEM((devices, main, cap), bf16),
            pltpu.VMEM((devices, width - main, cap), bf16),
            pltpu.VMEM((devices, width - main, cap), bf16),
            pltpu.VMEM((devices, entries_two, seeds), jnp.int16),
            pltpu.VMEM((2, width, nodes), f32),
            pltpu.VMEM((devices // 2, rows_two // 2, seeds), f32),
            pltpu.VMEM((devices // 2, rows_two // 2, seeds), f32),
            pltpu.VMEM((devices // 2, rows_two // 2, seeds), f32),
            pltpu.VMEM((devices // 2, rows_two // 2, seeds), bf16),
            pltpu.VMEM((devices // 2, rows_two // 2, seeds), bf16),
            pltpu.VMEM((devices // 16, rows_two // 2, seeds), bf16),
            pltpu.VMEM((devices // 16, rows_two // 2, seeds), bf16),
            pltpu.SemaphoreType.DMA((12,)),
            pltpu.SemaphoreType.DMA,
            pltpu.SemaphoreType.DMA((9,)),
            pltpu.SemaphoreType.DMA((6,)),
            pltpu.SemaphoreType.DMA((2, len(GROUPS) - 1)),
            pltpu.SemaphoreType.DMA((6,)),
            pltpu.SemaphoreType.DMA((devices // 16,)),
            pltpu.SemaphoreType.DMA((4,)),
            pltpu.SemaphoreType.DMA((2, 4)),
        ],
        compiler_params=pltpu.CompilerParams(
            vmem_limit_bytes=63 * MIB, collective_id=0, has_side_effects=True
        ),
    )(
        table_t,
        req_rows[:, None, :],
        req2_rows[:, None, :],
        count1,
        count2,
        frontier_list,
        seed_list,
        w1_self.T,
        w1_neigh.T,
        bias1[None, :],
        w2_self,
        w2_neigh,
    )
    return logits + bias2[:, None]


def solution(mesh):
    in_specs = (
        P(None, AXES),
        P(AXES, None),
        P(AXES),
        P(None, AXES),
        P(AXES, None),
        P(AXES),
        P(None, AXES),
        P(),
        P(),
        P(),
        P(),
        P(),
        P(),
    )
    return jax.shard_map(
        body, mesh=mesh, in_specs=in_specs, out_specs=P(None, AXES), check_vma=False
    )
```

```python
import functools

import jax
import jax.numpy as jnp
from jax import lax
from jax.experimental import pallas as pl
from jax.experimental.pallas import tpu as pltpu
from jax.sharding import PartitionSpec as P

AXES = ("shard", "grp")
LANES = 128
MIB = 1024 * 1024
MATRIX_LIMIT = 4 * MIB
EARLY = 2
GROUPS = (0, 16, 24, 30, 32)
BRIDGE = 2


FIELDS = 8
FIELD_BITS = 4


def tile(i, size=LANES):
    return pl.ds(pl.multiple_of(i * size, size), size)


def dot32(a, b):
    return jnp.dot(a, b, preferred_element_type=jnp.float32)


def tile_names(span):
    first = lax.broadcasted_iota(jnp.int32, (16, LANES), 0).astype(jnp.float32)
    return [(first + float(16 * b)).astype(jnp.bfloat16) for b in range(span // 16)]


def hits(row, names):
    few = jnp.broadcast_to(row, (16, row.shape[1])).astype(jnp.bfloat16)
    one, zero = jnp.ones((), jnp.bfloat16), jnp.zeros((), jnp.bfloat16)
    return [jnp.where(few == name, one, zero) for name in names]


def prepare_list(list_ref, key_ref, unit_ref, first_ref, cap):
    words = cap // FIELDS
    entry = list_ref[...]
    owner, slot = entry >> (cap.bit_length() - 1), entry & (cap - 1)
    key_ref[...] = owner * words + (slot & (words - 1))
    unit_ref[...] = jnp.ones((), jnp.int32) << (FIELD_BITS * (slot >> (words.bit_length() - 1)))
    first_ref[...] = entry[0:1].astype(jnp.float32)


def count_tile(key_ref, unit_ref, first, name, names, own_ref, near_ref, own_at, near_at, cols, to):
    words = name.shape[0]
    total = jnp.zeros(name.shape, jnp.int32)
    for k in range(1, key_ref.shape[0]):
        total = total + jnp.where(key_ref[k : k + 1, cols] == name, unit_ref[k : k + 1, cols], 0)
    for b in range(FIELDS):
        field = (total >> (FIELD_BITS * b)) & (2**FIELD_BITS - 1)
        near_ref[to, pl.ds(pl.multiple_of(near_at + b * words, words), words), :] = field.astype(
            jnp.float32
        ).astype(jnp.bfloat16)
    for b, part in enumerate(hits(first, names)):
        own_ref[to, pl.ds(pl.multiple_of(own_at + b * 16, 16), 16), :] = part


def count_slots(key_ref, unit_ref, first_ref, own_ref, near_ref, cap, owner_of, first, last):
    across = key_ref.shape[1] // LANES
    some = 4 if across % 4 == 0 else 1
    words = cap // FIELDS
    names = tile_names(cap)
    low = lax.broadcasted_iota(jnp.int32, (words, LANES), 0)

    def one(i, carry):
        at, base = lax.div(i, across // some), lax.rem(i, across // some) * some
        owner = owner_of(at)
        name, start = low + owner * words, (owner * cap).astype(jnp.float32)
        for c in range(some):
            cols = tile(base + c)
            own = first_ref[0:1, cols] - start
            count_tile(
                key_ref, unit_ref, own, name, names, own_ref, near_ref, at * cap, at * cap, cols, base + c
            )
        return carry

    lax.fori_loop(first * (across // some), last * (across // some), one, 0)


def select_seeds(lists_ref, key_ref, unit_ref, first_ref, out_ref, me, cap, first, last):
    devices, _, seeds = lists_ref.shape
    depth = devices // 8

    def step_at(at):
        core, y = lax.div(at, 4 * depth), lax.rem(lax.div(at, 2 * depth), 2)
        return core + 2 * y + 4 * lax.rem(lax.div(at, depth), 2) + 8 * lax.rem(at, depth)

    words = cap // FIELDS
    names = tile_names(cap)
    low = lax.broadcasted_iota(jnp.int32, (words, LANES), 0)

    def one(at, carry):
        local = lists_ref[at].astype(jnp.int32) - me * cap
        field = local >> (words.bit_length() - 1)
        here = jnp.logical_and(field >= 0, field < FIELDS)
        key_ref[...] = local & (words - 1)
        unit_ref[...] = jnp.where(here, jnp.ones((), jnp.int32) << (FIELD_BITS * (field & (FIELDS - 1))), 0)
        first_ref[...] = local[0:1].astype(jnp.float32)
        for c in range(seeds // LANES):
            cols = slice(c * LANES, (c + 1) * LANES)
            to = step_at(at) * (seeds // LANES) + c
            count_tile(
                key_ref, unit_ref, first_ref[0:1, cols], low, names, out_ref, out_ref, 0, cap, cols, to
            )
        return carry

    lax.fori_loop(first, last, one, 0)


def onehot_slots(asked_ref, out_ref, cap, first, last):
    nodes = out_ref.shape[1]
    names = tile_names(LANES)

    def one(t, carry):
        wanted = asked_ref[t].astype(jnp.float32)
        for b in range(nodes // LANES):
            for c, part in enumerate(hits(wanted - float(b * LANES), names)):
                out_ref[t, b * LANES + 16 * c : b * LANES + 16 * c + 16, :] = part
        return carry

    lax.fori_loop(first, last, one, 0)


def whole_kernel(grp, rows_two, *refs):
    req_hbm, req2_hbm, front_hbm, seed_hbm, w1s_hbm, w2s_hbm = (refs[k] for k in (1, 2, 5, 6, 7, 10))
    devices, cap, cap_two = req_hbm.shape[0], req_hbm.shape[2], req2_hbm.shape[2]
    nodes, seeds = front_hbm.shape[1], seed_hbm.shape[1]
    width, hidden_width = w1s_hbm.shape
    wide = -(-width // LANES) * LANES
    bf16 = jnp.bfloat16
    pl.run_scoped(
        functools.partial(inner_kernel, grp, *refs),
        pltpu.VMEM((hidden_width, 2 * wide), bf16),
        pltpu.VMEM((rows_two, hidden_width), bf16),
        pltpu.VMEM((nodes // LANES, devices * cap, LANES), bf16),
        pltpu.VMEM((nodes // LANES, devices * cap, LANES), bf16),
        pltpu.VMEM((devices, nodes, LANES), bf16),
        pltpu.VMEM((devices * seeds // LANES, 2 * cap_two, LANES), bf16),
        pltpu.VMEM((devices, -(-width // 16) * 16, cap), bf16),
        pltpu.VMEM((nodes // LANES, 2 * wide, LANES), bf16),
        pltpu.VMEM((nodes // LANES, rows_two, LANES), bf16),
        pltpu.VMEM((devices // 2, 2, rows_two // 2, 2 * cap_two), bf16),
    )


def inner_kernel(
    grp,
    table_hbm,
    req_hbm,
    req2_hbm,
    count1_hbm,
    count2_hbm,
    front_hbm,
    seed_hbm,
    w1s_hbm,
    w1n_hbm,
    bias1_hbm,
    w2s_hbm,
    w2n_hbm,
    out_ref,
    table,
    req_ref,
    req2_ref,
    count1_ref,
    count2_ref,
    front_ref,
    seed_ref,
    w1s_ref,
    w1n_ref,
    bias1_ref,
    w2s_ref,
    w2n_ref,
    key1,
    unit1,
    first1,
    key2,
    unit2,
    first2,
    asked,
    ids,
    rows,
    block,
    send,
    got,
    send_rest,
    got_rest,
    lists,
    acc,
    term_out,
    term_in,
    term,
    send2,
    got2,
    bridge_out,
    bridge_in,
    load_sems,
    in_sems,
    group_sems,
    cross_sems,
    bridge_sems,
    ask_sems,
    list_sems,
    w1,
    w2,
    own,
    near,
    onehot,
    select,
    flat,
    pair,
    payload,
    chosen,
):
    devices, _, cap = req_ref.shape
    cap_two = req2_ref.shape[2]
    me = lax.axis_index(AXES[0]) * grp + lax.axis_index(AXES[1])
    half = devices // 2
    bits = devices.bit_length() - 1

    def peer(t):
        total = 0
        for i in range(bits):
            mine = lax.rem(lax.div(me, 2**i), 2)
            if isinstance(t, int):
                bit = 1 - mine if (t >> i) & 1 else mine
            else:
                other = lax.rem(lax.div(t, 2**i), 2)
                bit = mine + other - 2 * mine * other
            total = total + bit * 2**i
        return total

    def step_of(p):
        return half * (1 - lax.rem(p, 2)) + lax.div(p, 2)

    def coordinates(to):
        return (lax.div(to, grp), lax.rem(to, grp))

    def place(t):
        return coordinates(peer(t))

    def remote(src, dst, out_sem, in_sem, to):
        return pltpu.make_async_remote_copy(
            src_ref=src,
            dst_ref=dst,
            send_sem=out_sem,
            recv_sem=in_sem,
            device_id=coordinates(to),
            device_id_type=pl.DeviceIdType.MESH,
        )

    steps = [devices * k // 32 for k in GROUPS]

    def group_of(p):
        return sum((p >= edge) * 1 if isinstance(p, int) else (p >= edge).astype(jnp.int32) for edge in steps[1:-1])

    def feature(to, t, p):
        group = group_of(p)
        remote(send.at[t], got.at[p], load_sems.at[9], group_sems.at[0, group], to).start()
        remote(
            send_rest.at[t], got_rest.at[p], load_sems.at[10], group_sems.at[1, group], to
        ).start()

    def arrived(first, last):
        count = last - first - (first <= 1 < last)
        group = group_of(first)
        some = pl.ds(0, count)
        remote(
            send.at[some], got.at[some], load_sems.at[9], group_sems.at[0, group], peer(1)
        ).wait_recv()
        remote(
            send_rest.at[some], got_rest.at[some], load_sems.at[10], group_sems.at[1, group], peer(1)
        ).wait_recv()

    pairs = (
        (front_hbm, front_ref),
        (req_hbm, req_ref),
        (req2_hbm, req2_ref),
        (table_hbm, table),
        (w1s_hbm, w1s_ref),
        (w1n_hbm, w1n_ref),
        (bias1_hbm, bias1_ref),
        (w2s_hbm, w2s_ref),
        (w2n_hbm, w2n_ref),
        (seed_hbm, seed_ref),
        (count1_hbm, count1_ref),
        (count2_hbm, count2_ref),
    )
    loads = [pltpu.make_async_copy(a, b, load_sems.at[i]) for i, (a, b) in enumerate(pairs)]
    for load in loads[:4]:
        load.start()
    barrier = pltpu.get_barrier_semaphore()
    for t in range(devices - 1, 0, -1):
        pl.semaphore_signal(
            barrier, inc=1, device_id=place(t), device_id_type=pl.DeviceIdType.MESH
        )
    for load in loads[4:]:
        load.start()
    loads[0].wait()
    prepare_list(front_ref, key1, unit1, first1, cap)
    loads[1].wait()
    loads[2].wait()
    for load in loads[9:]:
        load.wait()
    entry = seed_ref[...]
    owner, slot = entry >> (cap_two.bit_length() - 1), entry & (cap_two - 1)

    limit = jnp.zeros_like(entry)
    for o in range(devices):
        limit = jnp.where(owner == o, count2_ref[o], limit)
    live = slot < limit
    lists[0] = jnp.where(live, entry, -1).astype(lists.dtype)
    early = devices * EARLY // 32

    def owner_at(p):
        return peer(step_of(p))

    count_slots(key1, unit1, first1, own, near, cap, owner_at, 0, early)
    loads[3].wait()
    step = 4 * LANES if rows.shape[0] % (4 * LANES) == 0 else LANES

    def transpose(i, carry):
        rows[tile(i, step), :] = table[:, tile(i, step)].T.astype(jnp.float32)
        return carry

    pieces = rows.shape[0] // step
    first_piece, second_piece = pieces // 8, pieces // 2
    lax.fori_loop(0, first_piece, transpose, 0)
    pl.semaphore_wait(barrier, devices - 1)

    couples = devices // 2

    def ask(t):
        quarter = t % half // (half // 4)
        return remote(req_ref.at[peer(t)], ids.at[t], load_sems.at[0], ask_sems.at[quarter], peer(t))

    def ask_two(t):
        return remote(req2_ref.at[peer(t)], asked.at[t], load_sems.at[1], in_sems.at[0], peer(t))

    def hand_on(k):
        depth = devices // 8
        if k == 0:
            return [
                remote(lists.at[0], lists.at[j], load_sems.at[2], list_sems.at[0], peer(8 * j))
                for j in range(1, depth)
            ]
        count = depth << (k - 1)
        return [
            remote(
                lists.at[pl.ds(0, count)],
                lists.at[pl.ds(count, count)],
                load_sems.at[2],
                list_sems.at[k],
                peer(8 >> k),
            )
        ]

    def take(k):
        if k == 0:
            some = pl.ds(0, devices // 8 - 1)
            remote(
                lists.at[some], lists.at[some], load_sems.at[2], list_sems.at[0], peer(1)
            ).wait()
        else:
            hand_on(k)[0].wait()

    for t in sorted(range(1, devices), key=lambda t: (t % half // (half // 4), -t)):
        ask(t).start()
    own_ids = pltpu.make_async_copy(req_ref.at[me], ids.at[0], load_sems.at[3])
    own_ids.start()
    for t in range(devices - 1, 0, -1):
        ask_two(t).start()
    asked[0] = req2_ref[me]
    for one in hand_on(0):
        one.start()
    lax.fori_loop(first_piece, second_piece, transpose, 0)
    lax.fori_loop(second_piece, pieces, transpose, 0)
    own_ids.wait()
    rest = pl.ds(1, devices - 1)

    def asked_for(count, k):
        some = pl.ds(0, count)
        return remote(req_ref.at[some], ids.at[some], load_sems.at[0], ask_sems.at[k], peer(1))

    asked_for(half // 2 - 1, 0).wait_recv()

    main = send.shape[1]

    def pick(t, at):
        for j in range(cap):
            block[at, j : j + 1, :] = rows[pl.ds(ids[t, 0, j], 1), :]
        columns = block[at].T.astype(jnp.bfloat16)
        return columns[:main], columns[main:]

    def put(to, rest, at, columns):
        to[at], rest[at] = columns

    def pick_and_send(i, carry):
        to, before = peer(i), peer(i - 1)
        put(send, send_rest, half + i, pick(half + i, 0))
        put(send, send_rest, i, pick(i, 1))
        feature(lax.rem(before + half, devices), half + i - 1, 2 * i - 2)
        feature(before, i - 1, 2 * i - 1)
        return carry

    put(send, send_rest, half, pick(half, 0))
    put(send, send_rest, half + 1, pick(half + 1, 1))
    feature(peer(half), half, 0)
    put(send, send_rest, 1, pick(1, 0))
    put(got, got_rest, 1, pick(0, 1))
    lax.fori_loop(2, half // 4, pick_and_send, 0)
    take(0)
    hand_on(1)[0].start()
    for k in range(1, 4):
        asked_for(half // 2, k).wait_recv()
        lax.fori_loop(k * half // 4, (k + 1) * half // 4, pick_and_send, 0)
    asked_for(devices - 1, 0).wait_send()
    remote(req2_ref.at[rest], asked.at[rest], load_sems.at[1], in_sems.at[0], peer(1)).wait()
    onehot_slots(asked, onehot, cap_two, 0, 2)
    feature(peer(devices - 1), devices - 1, devices - 2)
    feature(peer(half - 1), half - 1, devices - 1)
    onehot_slots(asked, onehot, cap_two, 2, devices)
    for load in loads[4:9]:
        load.wait()
    width, hidden_width = w1s_ref.shape[0], w1.shape[0]
    wide = w1.shape[1] // 2
    classes, half_rows = w2s_ref.shape[0], w2.shape[0] // 2
    w1[...] = jnp.zeros_like(w1)
    w1[:, :width] = w1s_ref[...].T
    w1[:, wide : wide + width] = w1n_ref[...].T
    w2[...] = jnp.zeros_like(w2)
    w2[:classes] = w2s_ref[...]
    w2[half_rows : half_rows + classes] = w2n_ref[...]
    pair[...] = jnp.zeros_like(pair)
    bias1 = jnp.broadcast_to(bias1_ref[...], (8, hidden_width)).T[:, :1]

    take(1)
    hand_on(2)[0].start()
    count_slots(key1, unit1, first1, own, near, cap, owner_at, early, devices * 5 // 8)
    take(2)
    hand_on(3)[0].start()
    count_slots(key1, unit1, first1, own, near, cap, owner_at, devices * 5 // 8, devices)
    take(3)
    select_seeds(lists, key2, unit2, first2, select, me, cap_two, 0, devices)
    nodes = own.shape[0] * LANES
    chunk = 2 * LANES
    def lay(p, carry):
        count = count1_ref[owner_at(p)]
        for part, at, rows_here in ((got, 0, main), (got_rest, main, got_rest.shape[1])):
            slot = lax.broadcasted_iota(jnp.int32, part.shape[1:], 1)
            live = jnp.where(slot < count, part[p].astype(jnp.float32), 0.0)
            flat[p, at : at + rows_here, :] = live.astype(jnp.bfloat16)
        return carry

    def arrive(first, last):
        arrived(first, last)
        lax.fori_loop(first, last, lay, 0)

    arrive(0, steps[1])

    def side_by_side(parts):
        return jnp.concatenate(parts, axis=1)

    def picked(matrix, c, first, last):
        left = side_by_side([flat[p, :width, :] for p in range(first, last)])
        some = range(c * chunk // LANES, (c + 1) * chunk // LANES)
        return dot32(left, side_by_side([matrix[n, first * cap : last * cap, :] for n in some]))

    def add_up(first, last, fresh):
        for c in range(nodes // chunk):
            cols = slice(c * chunk, (c + 1) * chunk)
            for m, matrix in enumerate((own, near)):
                part = picked(matrix, c, first, last)
                acc[m, :, cols] = part if fresh else acc[m, :, cols] + part

    add_up(0, steps[1], True)
    for first, last in zip(steps[1:-2], steps[2:-1]):
        arrive(first, last)
        add_up(first, last, False)
    fan_two, fan_one = 1.0 / (front_ref.shape[0] - 1), 1.0 / (seed_ref.shape[0] - 1)
    arrive(steps[-2], steps[-1])
    scale = jnp.where(lax.broadcasted_iota(jnp.int32, (w2.shape[0], 1), 0) < half_rows, 1.0, fan_one)
    for c in range(nodes // chunk):
        cols = slice(c * chunk, (c + 1) * chunk)
        mine = acc[0, :, cols] + picked(own, c, steps[-2], steps[-1])
        summed = (acc[1, :, cols] + picked(near, c, steps[-2], steps[-1])) * fan_two
        for n in range(chunk // LANES):
            at, lanes = c * chunk // LANES + n, slice(n * LANES, (n + 1) * LANES)
            pair[at, :width, :] = mine[:, lanes].astype(jnp.bfloat16)
            pair[at, wide : wide + width, :] = summed[:, lanes].astype(jnp.bfloat16)
    hidden = []
    for c in range(nodes // chunk):
        some = range(c * chunk // LANES, (c + 1) * chunk // LANES)
        preact = dot32(w1[...], side_by_side([pair[n] for n in some])) + bias1
        hidden.append(jnp.maximum(preact, 0.0).astype(jnp.bfloat16))
    for c in range(nodes // chunk):
        last = (dot32(w2[...], hidden[c]) * scale).astype(jnp.bfloat16)
        for n in range(chunk // LANES):
            payload[c * chunk // LANES + n] = last[:, n * LANES : (n + 1) * LANES]
    across = term.shape[2] // LANES

    def choose(b):
        left = side_by_side([payload[n] for n in range(nodes // LANES)])
        for i in batches[b]:
            both = dot32(left, side_by_side([onehot[2 * i], onehot[2 * i + 1]])).astype(jnp.bfloat16)
            for c in range(2):
                cols = slice(c * cap_two, (c + 1) * cap_two)
                chosen[i, c, :, :cap_two] = both[:half_rows, cols]
                chosen[i, c, :, cap_two:] = both[half_rows:, cols]

    def terms(i):
        for c, out in ((1, term_out), (0, term)):
            at = (2 * i + c) * across
            out[i] = dot32(chosen[i, c], side_by_side([select[at + n] for n in range(across)]))

    moved, kept, direct = [], [], []
    for i in range(couples // 2, couples):
        (direct if i & 1 else moved if i & BRIDGE else kept).append(i)
    moved = [i ^ BRIDGE for i in kept]
    near_ones = [*range(couples // 4, couples // 2), *range(1, couples // 4), 0]
    middle, some = len(near_ones) // 2, len(direct) // 2
    batches = (moved, direct[:some], direct[some:], kept, near_ones[:middle], near_ones[middle:])

    def prepare(b):
        for i in batches[b]:
            terms(i)
        for i in batches[b]:
            remote(
                term_out.at[i], term_in.at[i], load_sems.at[11], cross_sems.at[b], peer(1)
            ).start()

    def crossed(b):
        some = pl.ds(0, len(batches[b]))
        remote(
            term_out.at[some], term_in.at[some], load_sems.at[11], cross_sems.at[b], peer(1)
        ).wait_recv()

    def bridge(k):
        return remote(
            bridge_out.at[k], bridge_in.at[k], load_sems.at[4], bridge_sems.at[k], peer(2 * BRIDGE)
        )

    def away(i):
        return remote(send2.at[i], got2.at[i], load_sems.at[5], in_sems.at[1], peer(2 * i))

    def join(i):
        send2[i] = (term[i] + term_in[i]).astype(jnp.bfloat16)

    def join_and_send(b):
        for i in batches[b]:
            if i > 0:
                join(i)
        for i in batches[b]:
            if i > 0:
                away(i).start()

    choose(0)
    choose(1)
    prepare(0)
    choose(2)
    prepare(1)
    crossed(0)
    for k, i in enumerate(moved):
        bridge_out[k] = (term[i] + term_in[i]).astype(jnp.bfloat16)
    for k in range(len(moved)):
        bridge(k).start()
    choose(4)
    prepare(2)
    crossed(1)
    join_and_send(1)
    choose(3)
    prepare(4)
    choose(5)
    prepare(3)
    crossed(2)
    join_and_send(2)
    prepare(5)
    crossed(4)
    join_and_send(4)
    crossed(3)
    for i in kept:
        term[i] = term[i] + term_in[i]
    crossed(5)
    join_and_send(5)
    for k, i in enumerate(kept):
        bridge(k).wait_recv()
        send2[i] = (term[i] + bridge_in[k].astype(jnp.float32)).astype(jnp.bfloat16)
    for i in kept:
        away(i).start()
    total = term[0] + term_in[0]
    arriving = direct + kept + near_ones[:-1]
    for src, dst, k, sent in (
        (send, got, 9, devices - 1),
        (send_rest, got_rest, 10, devices - 1),
        (term_out, term_in, 11, couples),
        (bridge_out, bridge_in, 4, len(moved)),
        (send2, got2, 5, len(arriving)),
    ):
        whole = remote(src.at[pl.ds(0, sent)], dst.at[pl.ds(0, sent)], load_sems.at[k], in_sems.at[1], peer(1))
        if k == 5:
            whole.wait()
        else:
            whole.wait_send()
    for i in arriving:
        total = total + got2[i].astype(jnp.float32)
    out_ref[...] = total[:classes]


def mask_rows(received, counts, capacity):
    is_live = (jnp.arange(capacity, dtype=jnp.int32)[None, :] < counts[:, None]).reshape(-1)
    flat = received.reshape(-1, received.shape[-1])
    return jnp.where(is_live[:, None], flat, jnp.zeros((), flat.dtype))


def right_product(rows, weight):
    return lax.dot_general(
        rows, weight, (((1,), (1,)), ((), ())), preferred_element_type=jnp.float32
    )


def take_body(
    table_t,
    req_rows,
    count1,
    frontier_list,
    req2_rows,
    count2,
    seed_list,
    w1_self,
    w1_neigh,
    bias1,
    w2_self,
    w2_neigh,
    bias2,
):
    feat_width = table_t.shape[0]
    capacity = req_rows.shape[1]
    table_rows = table_t.T
    picked_rows = jnp.take(
        table_rows,
        lax.all_to_all(req_rows, AXES, split_axis=0, concat_axis=0, tiled=True),
        axis=0,
    )
    received = lax.all_to_all(
        picked_rows, AXES, split_axis=0, concat_axis=0, tiled=True
    )
    flat = mask_rows(received, count1, capacity)
    fanout_two = frontier_list.shape[0] - 1
    front_nodes = frontier_list.shape[1]
    picked = jnp.take(flat, frontier_list.reshape(-1), axis=0).reshape(
        fanout_two + 1, front_nodes, feat_width
    )
    summed = (jnp.sum(picked[1:].astype(jnp.float32), axis=0) / fanout_two).astype(jnp.bfloat16)
    preact = right_product(picked[0], w1_self) + right_product(summed, w1_neigh) + bias1[None, :]
    hidden_rows = jax.nn.relu(preact).astype(jnp.bfloat16)
    cap_two = req2_rows.shape[1]
    payload = jnp.concatenate(
        [right_product(hidden_rows, w2_self), right_product(hidden_rows, w2_neigh)], axis=1
    )
    chosen = jnp.take(
        payload,
        lax.all_to_all(req2_rows, AXES, split_axis=0, concat_axis=0, tiled=True),
        axis=0,
    )
    got_back = lax.all_to_all(chosen, AXES, split_axis=0, concat_axis=0, tiled=True)
    flat_two = mask_rows(got_back, count2, cap_two)
    fanout_one = seed_list.shape[0] - 1
    seed_nodes = seed_list.shape[1]
    picked_two = jnp.take(flat_two, seed_list.reshape(-1), axis=0).reshape(
        fanout_one + 1, seed_nodes, flat_two.shape[1]
    )
    classes = w2_self.shape[0]
    near = jnp.sum(picked_two[1:, :, classes:], axis=0) / fanout_one
    logits = (picked_two[0, :, :classes] + near).T + bias2[:, None]
    return logits


def body(
    table_t,
    req_rows,
    count1,
    frontier_list,
    req2_rows,
    count2,
    seed_list,
    w1_self,
    w1_neigh,
    bias1,
    w2_self,
    w2_neigh,
    bias2,
):
    devices, cap = req_rows.shape
    cap_two = req2_rows.shape[1]
    nodes = frontier_list.shape[1]
    small = devices * max(cap, cap_two) * nodes <= MATRIX_LIMIT
    even = devices >= 32 and devices & (devices - 1) == 0
    plain = cap == cap_two == LANES and nodes % (2 * LANES) == 0
    plain = plain and table_t.shape[0] > 16
    few = max(frontier_list.shape[0], seed_list.shape[0]) <= 2**FIELD_BITS
    if not (small and even and plain and few):
        return take_body(
            table_t,
            req_rows,
            count1,
            frontier_list,
            req2_rows,
            count2,
            seed_list,
            w1_self,
            w1_neigh,
            bias1,
            w2_self,
            w2_neigh,
            bias2,
        )
    width, table_rows = table_t.shape
    entries, entries_two = frontier_list.shape[0], seed_list.shape[0]
    seeds = seed_list.shape[1]
    hidden_width, classes = w1_self.shape[0], w2_self.shape[0]
    rows_two = 2 * (-(-classes // 16) * 16)
    bf16, f32, i32 = jnp.bfloat16, jnp.float32, jnp.int32
    main = (width - 1) // 16 * 16
    logits = pl.pallas_call(
        functools.partial(whole_kernel, lax.axis_size(AXES[1]), rows_two),
        in_specs=[pl.BlockSpec(memory_space=pl.ANY)] * 12,
        out_specs=pl.BlockSpec(memory_space=pltpu.VMEM),
        out_shape=pltpu.VMEM((classes, seeds), f32),
        scratch_shapes=[
            pltpu.VMEM((width, table_rows), bf16),
            pltpu.VMEM((devices, 1, cap), i32),
            pltpu.VMEM((devices, 1, cap_two), i32),
            pltpu.SMEM((devices,), i32),
            pltpu.SMEM((devices,), i32),
            pltpu.VMEM((entries, nodes), i32),
            pltpu.VMEM((entries_two, seeds), i32),
            pltpu.VMEM((width, hidden_width), bf16),
            pltpu.VMEM((width, hidden_width), bf16),
            pltpu.VMEM((1, hidden_width), f32),
            pltpu.VMEM((classes, hidden_width), bf16),
            pltpu.VMEM((classes, hidden_width), bf16),
            pltpu.VMEM((entries, nodes), i32),
            pltpu.VMEM((entries, nodes), i32),
            pltpu.VMEM((1, nodes), f32),
            pltpu.VMEM((entries_two, seeds), i32),
            pltpu.VMEM((entries_two, seeds), i32),
            pltpu.VMEM((1, seeds), f32),
            pltpu.VMEM((devices, 1, cap_two), i32),
            pltpu.SMEM((devices, 1, cap), i32),
            pltpu.VMEM((table_rows, width), f32),
            pltpu.VMEM((2, cap, width), f32),
            pltpu.VMEM((devices, main, cap), bf16),
            pltpu.VMEM((devices, main, cap), bf16),
            pltpu.VMEM((devices, width - main, cap), bf16),
            pltpu.VMEM((devices, width - main, cap), bf16),
            pltpu.VMEM((devices, entries_two, seeds), jnp.int16),
            pltpu.VMEM((2, width, nodes), f32),
            pltpu.VMEM((devices // 2, rows_two // 2, seeds), f32),
            pltpu.VMEM((devices // 2, rows_two // 2, seeds), f32),
            pltpu.VMEM((devices // 2, rows_two // 2, seeds), f32),
            pltpu.VMEM((devices // 2, rows_two // 2, seeds), bf16),
            pltpu.VMEM((devices // 2, rows_two // 2, seeds), bf16),
            pltpu.VMEM((devices // 16, rows_two // 2, seeds), bf16),
            pltpu.VMEM((devices // 16, rows_two // 2, seeds), bf16),
            pltpu.SemaphoreType.DMA((12,)),
            pltpu.SemaphoreType.DMA((2,)),
            pltpu.SemaphoreType.DMA((2, len(GROUPS) - 1)),
            pltpu.SemaphoreType.DMA((6,)),
            pltpu.SemaphoreType.DMA((devices // 16,)),
            pltpu.SemaphoreType.DMA((4,)),
            pltpu.SemaphoreType.DMA((4,)),
        ],
        compiler_params=pltpu.CompilerParams(
            vmem_limit_bytes=63 * MIB, collective_id=0, has_side_effects=True
        ),
    )(
        table_t,
        req_rows[:, None, :],
        req2_rows[:, None, :],
        count1,
        count2,
        frontier_list,
        seed_list,
        w1_self.T,
        w1_neigh.T,
        bias1[None, :],
        w2_self,
        w2_neigh,
    )
    return logits + bias2[:, None]


def solution(mesh):
    in_specs = (
        P(None, AXES),
        P(AXES, None),
        P(AXES),
        P(None, AXES),
        P(AXES, None),
        P(AXES),
        P(None, AXES),
        P(),
        P(),
        P(),
        P(),
        P(),
        P(),
    )
    return jax.shard_map(
        body, mesh=mesh, in_specs=in_specs, out_specs=P(None, AXES), check_vma=False
    )
```

```python
import functools

import jax
import jax.numpy as jnp
from jax import lax
from jax.experimental import pallas as pl
from jax.experimental.pallas import tpu as pltpu
from jax.sharding import PartitionSpec as P

AXES = ("shard", "grp")
LANES = 128
MIB = 1024 * 1024
MATRIX_LIMIT = 4 * MIB
EARLY = 2
GROUPS = (0, 16, 24, 30, 32)
BRIDGE = 2


FIELDS = 8
FIELD_BITS = 4


def tile(i, size=LANES):
    return pl.ds(pl.multiple_of(i * size, size), size)


def dot32(a, b):
    return jnp.dot(a, b, preferred_element_type=jnp.float32)


def tile_names(span):
    first = lax.broadcasted_iota(jnp.int32, (16, LANES), 0).astype(jnp.float32)
    return [(first + float(16 * b)).astype(jnp.bfloat16) for b in range(span // 16)]


def hits(row, names):
    few = jnp.broadcast_to(row, (16, row.shape[1])).astype(jnp.bfloat16)
    one, zero = jnp.ones((), jnp.bfloat16), jnp.zeros((), jnp.bfloat16)
    return [jnp.where(few == name, one, zero) for name in names]


def prepare_list(list_ref, key_ref, unit_ref, first_ref, cap):
    words = cap // FIELDS
    entry = list_ref[...]
    owner, slot = entry >> (cap.bit_length() - 1), entry & (cap - 1)
    key_ref[...] = owner * words + (slot & (words - 1))
    unit_ref[...] = jnp.ones((), jnp.int32) << (FIELD_BITS * (slot >> (words.bit_length() - 1)))
    first_ref[...] = entry[0:1].astype(jnp.float32)


def count_tile(key_ref, unit_ref, first, name, names, own_ref, near_ref, own_at, near_at, cols, to):
    words = name.shape[0]
    total = jnp.zeros(name.shape, jnp.int32)
    for k in range(1, key_ref.shape[0]):
        total = total + jnp.where(key_ref[k : k + 1, cols] == name, unit_ref[k : k + 1, cols], 0)
    for b in range(FIELDS):
        field = (total >> (FIELD_BITS * b)) & (2**FIELD_BITS - 1)
        near_ref[to, pl.ds(pl.multiple_of(near_at + b * words, words), words), :] = field.astype(
            jnp.float32
        ).astype(jnp.bfloat16)
    for b, part in enumerate(hits(first, names)):
        own_ref[to, pl.ds(pl.multiple_of(own_at + b * 16, 16), 16), :] = part


def count_slots(key_ref, unit_ref, first_ref, own_ref, near_ref, cap, owner_of, first, last):
    across = key_ref.shape[1] // LANES
    some = 4 if across % 4 == 0 else 1
    words = cap // FIELDS
    names = tile_names(cap)
    low = lax.broadcasted_iota(jnp.int32, (words, LANES), 0)

    def one(i, carry):
        at, base = lax.div(i, across // some), lax.rem(i, across // some) * some
        owner = owner_of(at)
        name, start = low + owner * words, (owner * cap).astype(jnp.float32)
        for c in range(some):
            cols = tile(base + c)
            own = first_ref[0:1, cols] - start
            count_tile(
                key_ref, unit_ref, own, name, names, own_ref, near_ref, at * cap, at * cap, cols, base + c
            )
        return carry

    lax.fori_loop(first * (across // some), last * (across // some), one, 0)


def select_seeds(lists_ref, key_ref, unit_ref, first_ref, out_ref, me, cap, first, last):
    devices, _, seeds = lists_ref.shape
    depth = devices // 8

    def step_at(at):
        core, y = lax.div(at, 4 * depth), lax.rem(lax.div(at, 2 * depth), 2)
        return core + 2 * y + 4 * lax.rem(lax.div(at, depth), 2) + 8 * lax.rem(at, depth)

    words = cap // FIELDS
    names = tile_names(cap)
    low = lax.broadcasted_iota(jnp.int32, (words, LANES), 0)

    def one(at, carry):
        local = lists_ref[at].astype(jnp.int32) - me * cap
        field = local >> (words.bit_length() - 1)
        here = jnp.logical_and(field >= 0, field < FIELDS)
        key_ref[...] = local & (words - 1)
        unit_ref[...] = jnp.where(here, jnp.ones((), jnp.int32) << (FIELD_BITS * (field & (FIELDS - 1))), 0)
        first_ref[...] = local[0:1].astype(jnp.float32)
        for c in range(seeds // LANES):
            cols = slice(c * LANES, (c + 1) * LANES)
            to = step_at(at) * (seeds // LANES) + c
            count_tile(
                key_ref, unit_ref, first_ref[0:1, cols], low, names, out_ref, out_ref, 0, cap, cols, to
            )
        return carry

    lax.fori_loop(first, last, one, 0)


def onehot_slots(asked_ref, out_ref, cap, first, last):
    nodes = out_ref.shape[1]
    names = tile_names(LANES)

    def one(t, carry):
        wanted = asked_ref[t].astype(jnp.float32)
        for b in range(nodes // LANES):
            for c, part in enumerate(hits(wanted - float(b * LANES), names)):
                out_ref[t, b * LANES + 16 * c : b * LANES + 16 * c + 16, :] = part
        return carry

    lax.fori_loop(first, last, one, 0)


def whole_kernel(grp, rows_two, *refs):
    req_hbm, req2_hbm, front_hbm, seed_hbm, w1s_hbm, w2s_hbm = (refs[k] for k in (1, 2, 5, 6, 7, 10))
    devices, cap, cap_two = req_hbm.shape[0], req_hbm.shape[2], req2_hbm.shape[2]
    nodes, seeds = front_hbm.shape[1], seed_hbm.shape[1]
    width, hidden_width = w1s_hbm.shape
    wide = -(-width // LANES) * LANES
    bf16 = jnp.bfloat16
    pl.run_scoped(
        functools.partial(inner_kernel, grp, *refs),
        pltpu.VMEM((hidden_width, 2 * wide), bf16),
        pltpu.VMEM((rows_two, hidden_width), bf16),
        pltpu.VMEM((nodes // LANES, devices * cap, LANES), bf16),
        pltpu.VMEM((nodes // LANES, devices * cap, LANES), bf16),
        pltpu.VMEM((devices, nodes, LANES), bf16),
        pltpu.VMEM((devices * seeds // LANES, 2 * cap_two, LANES), bf16),
        pltpu.VMEM((devices, -(-width // 16) * 16, cap), bf16),
        pltpu.VMEM((nodes // LANES, 2 * wide, LANES), bf16),
        pltpu.VMEM((nodes // LANES, rows_two, LANES), bf16),
        pltpu.VMEM((devices // 2, 2, rows_two // 2, 2 * cap_two), bf16),
    )


def inner_kernel(
    grp,
    table_hbm,
    req_hbm,
    req2_hbm,
    count1_hbm,
    count2_hbm,
    front_hbm,
    seed_hbm,
    w1s_hbm,
    w1n_hbm,
    bias1_hbm,
    w2s_hbm,
    w2n_hbm,
    out_ref,
    table,
    req_ref,
    req2_ref,
    count1_ref,
    count2_ref,
    front_ref,
    seed_ref,
    w1s_ref,
    w1n_ref,
    bias1_ref,
    w2s_ref,
    w2n_ref,
    key1,
    unit1,
    first1,
    key2,
    unit2,
    first2,
    asked,
    ids,
    rows,
    block,
    send,
    got,
    send_rest,
    got_rest,
    lists,
    acc,
    term_out,
    term_in,
    term,
    send2,
    got2,
    bridge_out,
    bridge_in,
    load_sems,
    in_sems,
    group_sems,
    cross_sems,
    bridge_sems,
    ask_sems,
    list_sems,
    w1,
    w2,
    own,
    near,
    onehot,
    select,
    flat,
    pair,
    payload,
    chosen,
):
    devices, _, cap = req_ref.shape
    cap_two = req2_ref.shape[2]
    me = lax.axis_index(AXES[0]) * grp + lax.axis_index(AXES[1])
    half = devices // 2
    bits = devices.bit_length() - 1

    def peer(t):
        total = 0
        for i in range(bits):
            mine = lax.rem(lax.div(me, 2**i), 2)
            if isinstance(t, int):
                bit = 1 - mine if (t >> i) & 1 else mine
            else:
                other = lax.rem(lax.div(t, 2**i), 2)
                bit = mine + other - 2 * mine * other
            total = total + bit * 2**i
        return total

    def step_of(p):
        return half * (1 - lax.rem(p, 2)) + lax.div(p, 2)

    def coordinates(to):
        return (lax.div(to, grp), lax.rem(to, grp))

    def place(t):
        return coordinates(peer(t))

    def remote(src, dst, out_sem, in_sem, to):
        return pltpu.make_async_remote_copy(
            src_ref=src,
            dst_ref=dst,
            send_sem=out_sem,
            recv_sem=in_sem,
            device_id=coordinates(to),
            device_id_type=pl.DeviceIdType.MESH,
        )

    steps = [devices * k // 32 for k in GROUPS]

    def group_of(p):
        return sum((p >= edge) * 1 if isinstance(p, int) else (p >= edge).astype(jnp.int32) for edge in steps[1:-1])

    def feature(to, t, p):
        group = group_of(p)
        remote(send.at[t], got.at[p], load_sems.at[9], group_sems.at[0, group], to).start()
        remote(
            send_rest.at[t], got_rest.at[p], load_sems.at[10], group_sems.at[1, group], to
        ).start()

    def arrived(first, last):
        count = last - first - (first <= 1 < last)
        group = group_of(first)
        some = pl.ds(0, count)
        remote(
            send.at[some], got.at[some], load_sems.at[9], group_sems.at[0, group], peer(1)
        ).wait_recv()
        remote(
            send_rest.at[some], got_rest.at[some], load_sems.at[10], group_sems.at[1, group], peer(1)
        ).wait_recv()

    pairs = (
        (front_hbm, front_ref),
        (req_hbm, req_ref),
        (req2_hbm, req2_ref),
        (table_hbm, table),
        (w1s_hbm, w1s_ref),
        (w1n_hbm, w1n_ref),
        (bias1_hbm, bias1_ref),
        (w2s_hbm, w2s_ref),
        (w2n_hbm, w2n_ref),
        (seed_hbm, seed_ref),
        (count1_hbm, count1_ref),
        (count2_hbm, count2_ref),
    )
    loads = [pltpu.make_async_copy(a, b, load_sems.at[i]) for i, (a, b) in enumerate(pairs)]
    for load in loads[:4]:
        load.start()
    barrier = pltpu.get_barrier_semaphore()
    for t in range(devices - 1, 0, -1):
        pl.semaphore_signal(
            barrier, inc=1, device_id=place(t), device_id_type=pl.DeviceIdType.MESH
        )
    for load in loads[4:]:
        load.start()
    loads[0].wait()
    prepare_list(front_ref, key1, unit1, first1, cap)
    loads[1].wait()
    loads[2].wait()
    for load in loads[9:]:
        load.wait()
    entry = seed_ref[...]
    owner, slot = entry >> (cap_two.bit_length() - 1), entry & (cap_two - 1)

    limit = jnp.zeros_like(entry)
    for o in range(devices):
        limit = jnp.where(owner == o, count2_ref[o], limit)
    live = slot < limit
    lists[0] = jnp.where(live, entry, -1).astype(lists.dtype)
    early = devices * EARLY // 32

    def owner_at(p):
        return peer(step_of(p))

    count_slots(key1, unit1, first1, own, near, cap, owner_at, 0, early)
    loads[3].wait()
    step = 4 * LANES if rows.shape[0] % (4 * LANES) == 0 else LANES

    def transpose(i, carry):
        rows[tile(i, step), :] = table[:, tile(i, step)].T.astype(jnp.float32)
        return carry

    pieces = rows.shape[0] // step
    first_piece, second_piece = pieces // 8, pieces // 2
    lax.fori_loop(0, first_piece, transpose, 0)
    pl.semaphore_wait(barrier, devices - 1)

    couples = devices // 2

    def ask(t):
        quarter = t % half // (half // 4)
        return remote(req_ref.at[peer(t)], ids.at[t], load_sems.at[0], ask_sems.at[quarter], peer(t))

    def ask_two(t):
        return remote(req2_ref.at[peer(t)], asked.at[t], load_sems.at[1], in_sems.at[0], peer(t))

    def hand_on(k):
        depth = devices // 8
        if k == 0:
            return [
                remote(lists.at[0], lists.at[j], load_sems.at[2], list_sems.at[0], peer(8 * j))
                for j in range(1, depth)
            ]
        count = depth << (k - 1)
        return [
            remote(
                lists.at[pl.ds(0, count)],
                lists.at[pl.ds(count, count)],
                load_sems.at[2],
                list_sems.at[k],
                peer(8 >> k),
            )
        ]

    def take(k):
        if k == 0:
            some = pl.ds(0, devices // 8 - 1)
            remote(
                lists.at[some], lists.at[some], load_sems.at[2], list_sems.at[0], peer(1)
            ).wait()
        else:
            hand_on(k)[0].wait()

    for t in sorted(range(1, devices), key=lambda t: (t % half // (half // 4), -t)):
        ask(t).start()
    own_ids = pltpu.make_async_copy(req_ref.at[me], ids.at[0], load_sems.at[3])
    own_ids.start()
    for t in range(devices - 1, 0, -1):
        ask_two(t).start()
    asked[0] = req2_ref[me]
    for one in hand_on(0):
        one.start()
    lax.fori_loop(first_piece, second_piece, transpose, 0)
    lax.fori_loop(second_piece, pieces, transpose, 0)
    own_ids.wait()
    rest = pl.ds(1, devices - 1)

    def asked_for(count, k):
        some = pl.ds(0, count)
        return remote(req_ref.at[some], ids.at[some], load_sems.at[0], ask_sems.at[k], peer(1))

    asked_for(half // 2 - 1, 0).wait_recv()

    main = send.shape[1]

    def pick(t, at):
        for j in range(cap):
            block[at, j : j + 1, :] = rows[pl.ds(ids[t, 0, j], 1), :]
        columns = block[at].T.astype(jnp.bfloat16)
        return columns[:main], columns[main:]

    def put(to, rest, at, columns):
        to[at], rest[at] = columns

    def pick_and_send(i, carry):
        to, before = peer(i), peer(i - 1)
        put(send, send_rest, half + i, pick(half + i, 0))
        put(send, send_rest, i, pick(i, 1))
        feature(lax.rem(before + half, devices), half + i - 1, 2 * i - 2)
        feature(before, i - 1, 2 * i - 1)
        return carry

    put(send, send_rest, half, pick(half, 0))
    put(send, send_rest, half + 1, pick(half + 1, 1))
    feature(peer(half), half, 0)
    put(send, send_rest, 1, pick(1, 0))
    lax.fori_loop(2, half // 4, pick_and_send, 0)
    take(0)
    hand_on(1)[0].start()
    for k in range(1, 4):
        asked_for(half // 2, k).wait_recv()
        lax.fori_loop(k * half // 4, (k + 1) * half // 4, pick_and_send, 0)
    put(got, got_rest, 1, pick(0, 1))
    asked_for(devices - 1, 0).wait_send()
    remote(req2_ref.at[rest], asked.at[rest], load_sems.at[1], in_sems.at[0], peer(1)).wait()
    onehot_slots(asked, onehot, cap_two, 0, 2)
    feature(peer(devices - 1), devices - 1, devices - 2)
    feature(peer(half - 1), half - 1, devices - 1)
    onehot_slots(asked, onehot, cap_two, 2, devices)
    for load in loads[4:9]:
        load.wait()
    width, hidden_width = w1s_ref.shape[0], w1.shape[0]
    wide = w1.shape[1] // 2
    classes, half_rows = w2s_ref.shape[0], w2.shape[0] // 2
    w1[...] = jnp.zeros_like(w1)
    w1[:, :width] = w1s_ref[...].T
    w1[:, wide : wide + width] = w1n_ref[...].T
    w2[...] = jnp.zeros_like(w2)
    w2[:classes] = w2s_ref[...]
    w2[half_rows : half_rows + classes] = w2n_ref[...]
    pair[...] = jnp.zeros_like(pair)
    bias1 = jnp.broadcast_to(bias1_ref[...], (8, hidden_width)).T[:, :1]

    take(1)
    hand_on(2)[0].start()
    count_slots(key1, unit1, first1, own, near, cap, owner_at, early, devices * 5 // 8)
    take(2)
    hand_on(3)[0].start()
    count_slots(key1, unit1, first1, own, near, cap, owner_at, devices * 5 // 8, devices)
    take(3)
    select_seeds(lists, key2, unit2, first2, select, me, cap_two, 0, devices)
    nodes = own.shape[0] * LANES
    chunk = 2 * LANES
    def lay(p, carry):
        count = count1_ref[owner_at(p)]
        for part, at, rows_here in ((got, 0, main), (got_rest, main, got_rest.shape[1])):
            slot = lax.broadcasted_iota(jnp.int32, part.shape[1:], 1)
            live = jnp.where(slot < count, part[p].astype(jnp.float32), 0.0)
            flat[p, at : at + rows_here, :] = live.astype(jnp.bfloat16)
        return carry

    def arrive(first, last):
        arrived(first, last)
        lax.fori_loop(first, last, lay, 0)

    arrive(0, steps[1])

    def side_by_side(parts):
        return jnp.concatenate(parts, axis=1)

    def picked(matrix, c, first, last):
        left = side_by_side([flat[p, :width, :] for p in range(first, last)])
        some = range(c * chunk // LANES, (c + 1) * chunk // LANES)
        return dot32(left, side_by_side([matrix[n, first * cap : last * cap, :] for n in some]))

    def add_up(first, last, fresh):
        for c in range(nodes // chunk):
            cols = slice(c * chunk, (c + 1) * chunk)
            for m, matrix in enumerate((own, near)):
                part = picked(matrix, c, first, last)
                acc[m, :, cols] = part if fresh else acc[m, :, cols] + part

    add_up(0, steps[1], True)
    for first, last in zip(steps[1:-2], steps[2:-1]):
        arrive(first, last)
        add_up(first, last, False)
    fan_two, fan_one = 1.0 / (front_ref.shape[0] - 1), 1.0 / (seed_ref.shape[0] - 1)
    arrive(steps[-2], steps[-1])
    scale = jnp.where(lax.broadcasted_iota(jnp.int32, (w2.shape[0], 1), 0) < half_rows, 1.0, fan_one)
    for c in range(nodes // chunk):
        cols = slice(c * chunk, (c + 1) * chunk)
        mine = acc[0, :, cols] + picked(own, c, steps[-2], steps[-1])
        summed = (acc[1, :, cols] + picked(near, c, steps[-2], steps[-1])) * fan_two
        for n in range(chunk // LANES):
            at, lanes = c * chunk // LANES + n, slice(n * LANES, (n + 1) * LANES)
            pair[at, :width, :] = mine[:, lanes].astype(jnp.bfloat16)
            pair[at, wide : wide + width, :] = summed[:, lanes].astype(jnp.bfloat16)
    hidden = []
    for c in range(nodes // chunk):
        some = range(c * chunk // LANES, (c + 1) * chunk // LANES)
        preact = dot32(w1[...], side_by_side([pair[n] for n in some])) + bias1
        hidden.append(jnp.maximum(preact, 0.0).astype(jnp.bfloat16))
    for c in range(nodes // chunk):
        last = (dot32(w2[...], hidden[c]) * scale).astype(jnp.bfloat16)
        for n in range(chunk // LANES):
            payload[c * chunk // LANES + n] = last[:, n * LANES : (n + 1) * LANES]
    across = term.shape[2] // LANES

    def choose(b):
        left = side_by_side([payload[n] for n in range(nodes // LANES)])
        for i in batches[b]:
            both = dot32(left, side_by_side([onehot[2 * i], onehot[2 * i + 1]])).astype(jnp.bfloat16)
            for c in range(2):
                cols = slice(c * cap_two, (c + 1) * cap_two)
                chosen[i, c, :, :cap_two] = both[:half_rows, cols]
                chosen[i, c, :, cap_two:] = both[half_rows:, cols]

    def terms(i):
        for c, out in ((1, term_out), (0, term)):
            at = (2 * i + c) * across
            out[i] = dot32(chosen[i, c], side_by_side([select[at + n] for n in range(across)]))

    moved, kept, direct = [], [], []
    for i in range(couples // 2, couples):
        (direct if i & 1 else moved if i & BRIDGE else kept).append(i)
    moved = [i ^ BRIDGE for i in kept]
    near_ones = [*range(couples // 4, couples // 2), *range(1, couples // 4), 0]
    middle, some = len(near_ones) // 2, len(direct) // 2
    batches = (moved, direct[:some], direct[some:], kept, near_ones[:middle], near_ones[middle:])

    def prepare(b):
        for i in batches[b]:
            terms(i)
        for i in batches[b]:
            remote(
                term_out.at[i], term_in.at[i], load_sems.at[11], cross_sems.at[b], peer(1)
            ).start()

    def crossed(b):
        some = pl.ds(0, len(batches[b]))
        remote(
            term_out.at[some], term_in.at[some], load_sems.at[11], cross_sems.at[b], peer(1)
        ).wait_recv()

    def bridge(k):
        return remote(
            bridge_out.at[k], bridge_in.at[k], load_sems.at[4], bridge_sems.at[k], peer(2 * BRIDGE)
        )

    def away(i):
        return remote(send2.at[i], got2.at[i], load_sems.at[5], in_sems.at[1], peer(2 * i))

    def join(i):
        send2[i] = (term[i] + term_in[i]).astype(jnp.bfloat16)

    def join_and_send(b):
        for i in batches[b]:
            if i > 0:
                join(i)
        for i in batches[b]:
            if i > 0:
                away(i).start()

    choose(0)
    choose(1)
    prepare(0)
    choose(2)
    prepare(1)
    crossed(0)
    for k, i in enumerate(moved):
        bridge_out[k] = (term[i] + term_in[i]).astype(jnp.bfloat16)
    for k in range(len(moved)):
        bridge(k).start()
    choose(4)
    prepare(2)
    crossed(1)
    join_and_send(1)
    choose(3)
    prepare(4)
    choose(5)
    prepare(3)
    crossed(2)
    join_and_send(2)
    prepare(5)
    crossed(4)
    join_and_send(4)
    crossed(3)
    for i in kept:
        term[i] = term[i] + term_in[i]
    crossed(5)
    join_and_send(5)
    for k, i in enumerate(kept):
        bridge(k).wait_recv()
        send2[i] = (term[i] + bridge_in[k].astype(jnp.float32)).astype(jnp.bfloat16)
    for i in kept:
        away(i).start()
    total = term[0] + term_in[0]
    arriving = direct + kept + near_ones[:-1]
    for src, dst, k, sent in (
        (send, got, 9, devices - 1),
        (send_rest, got_rest, 10, devices - 1),
        (term_out, term_in, 11, couples),
        (bridge_out, bridge_in, 4, len(moved)),
        (send2, got2, 5, len(arriving)),
    ):
        whole = remote(src.at[pl.ds(0, sent)], dst.at[pl.ds(0, sent)], load_sems.at[k], in_sems.at[1], peer(1))
        if k == 5:
            whole.wait()
        else:
            whole.wait_send()
    for i in arriving:
        total = total + got2[i].astype(jnp.float32)
    out_ref[...] = total[:classes]


def mask_rows(received, counts, capacity):
    is_live = (jnp.arange(capacity, dtype=jnp.int32)[None, :] < counts[:, None]).reshape(-1)
    flat = received.reshape(-1, received.shape[-1])
    return jnp.where(is_live[:, None], flat, jnp.zeros((), flat.dtype))


def right_product(rows, weight):
    return lax.dot_general(
        rows, weight, (((1,), (1,)), ((), ())), preferred_element_type=jnp.float32
    )


def take_body(
    table_t,
    req_rows,
    count1,
    frontier_list,
    req2_rows,
    count2,
    seed_list,
    w1_self,
    w1_neigh,
    bias1,
    w2_self,
    w2_neigh,
    bias2,
):
    feat_width = table_t.shape[0]
    capacity = req_rows.shape[1]
    table_rows = table_t.T
    picked_rows = jnp.take(
        table_rows,
        lax.all_to_all(req_rows, AXES, split_axis=0, concat_axis=0, tiled=True),
        axis=0,
    )
    received = lax.all_to_all(
        picked_rows, AXES, split_axis=0, concat_axis=0, tiled=True
    )
    flat = mask_rows(received, count1, capacity)
    fanout_two = frontier_list.shape[0] - 1
    front_nodes = frontier_list.shape[1]
    picked = jnp.take(flat, frontier_list.reshape(-1), axis=0).reshape(
        fanout_two + 1, front_nodes, feat_width
    )
    summed = (jnp.sum(picked[1:].astype(jnp.float32), axis=0) / fanout_two).astype(jnp.bfloat16)
    preact = right_product(picked[0], w1_self) + right_product(summed, w1_neigh) + bias1[None, :]
    hidden_rows = jax.nn.relu(preact).astype(jnp.bfloat16)
    cap_two = req2_rows.shape[1]
    payload = jnp.concatenate(
        [right_product(hidden_rows, w2_self), right_product(hidden_rows, w2_neigh)], axis=1
    )
    chosen = jnp.take(
        payload,
        lax.all_to_all(req2_rows, AXES, split_axis=0, concat_axis=0, tiled=True),
        axis=0,
    )
    got_back = lax.all_to_all(chosen, AXES, split_axis=0, concat_axis=0, tiled=True)
    flat_two = mask_rows(got_back, count2, cap_two)
    fanout_one = seed_list.shape[0] - 1
    seed_nodes = seed_list.shape[1]
    picked_two = jnp.take(flat_two, seed_list.reshape(-1), axis=0).reshape(
        fanout_one + 1, seed_nodes, flat_two.shape[1]
    )
    classes = w2_self.shape[0]
    near = jnp.sum(picked_two[1:, :, classes:], axis=0) / fanout_one
    logits = (picked_two[0, :, :classes] + near).T + bias2[:, None]
    return logits


def body(
    table_t,
    req_rows,
    count1,
    frontier_list,
    req2_rows,
    count2,
    seed_list,
    w1_self,
    w1_neigh,
    bias1,
    w2_self,
    w2_neigh,
    bias2,
):
    devices, cap = req_rows.shape
    cap_two = req2_rows.shape[1]
    nodes = frontier_list.shape[1]
    small = devices * max(cap, cap_two) * nodes <= MATRIX_LIMIT
    even = devices >= 32 and devices & (devices - 1) == 0
    plain = cap == cap_two == LANES and nodes % (2 * LANES) == 0
    plain = plain and table_t.shape[0] > 16
    few = max(frontier_list.shape[0], seed_list.shape[0]) <= 2**FIELD_BITS
    if not (small and even and plain and few):
        return take_body(
            table_t,
            req_rows,
            count1,
            frontier_list,
            req2_rows,
            count2,
            seed_list,
            w1_self,
            w1_neigh,
            bias1,
            w2_self,
            w2_neigh,
            bias2,
        )
    width, table_rows = table_t.shape
    entries, entries_two = frontier_list.shape[0], seed_list.shape[0]
    seeds = seed_list.shape[1]
    hidden_width, classes = w1_self.shape[0], w2_self.shape[0]
    rows_two = 2 * (-(-classes // 16) * 16)
    bf16, f32, i32 = jnp.bfloat16, jnp.float32, jnp.int32
    main = (width - 1) // 16 * 16
    logits = pl.pallas_call(
        functools.partial(whole_kernel, lax.axis_size(AXES[1]), rows_two),
        in_specs=[pl.BlockSpec(memory_space=pl.ANY)] * 12,
        out_specs=pl.BlockSpec(memory_space=pltpu.VMEM),
        out_shape=pltpu.VMEM((classes, seeds), f32),
        scratch_shapes=[
            pltpu.VMEM((width, table_rows), bf16),
            pltpu.VMEM((devices, 1, cap), i32),
            pltpu.VMEM((devices, 1, cap_two), i32),
            pltpu.SMEM((devices,), i32),
            pltpu.SMEM((devices,), i32),
            pltpu.VMEM((entries, nodes), i32),
            pltpu.VMEM((entries_two, seeds), i32),
            pltpu.VMEM((width, hidden_width), bf16),
            pltpu.VMEM((width, hidden_width), bf16),
            pltpu.VMEM((1, hidden_width), f32),
            pltpu.VMEM((classes, hidden_width), bf16),
            pltpu.VMEM((classes, hidden_width), bf16),
            pltpu.VMEM((entries, nodes), i32),
            pltpu.VMEM((entries, nodes), i32),
            pltpu.VMEM((1, nodes), f32),
            pltpu.VMEM((entries_two, seeds), i32),
            pltpu.VMEM((entries_two, seeds), i32),
            pltpu.VMEM((1, seeds), f32),
            pltpu.VMEM((devices, 1, cap_two), i32),
            pltpu.SMEM((devices, 1, cap), i32),
            pltpu.VMEM((table_rows, width), f32),
            pltpu.VMEM((2, cap, width), f32),
            pltpu.VMEM((devices, main, cap), bf16),
            pltpu.VMEM((devices, main, cap), bf16),
            pltpu.VMEM((devices, width - main, cap), bf16),
            pltpu.VMEM((devices, width - main, cap), bf16),
            pltpu.VMEM((devices, entries_two, seeds), jnp.int16),
            pltpu.VMEM((2, width, nodes), f32),
            pltpu.VMEM((devices // 2, rows_two // 2, seeds), f32),
            pltpu.VMEM((devices // 2, rows_two // 2, seeds), f32),
            pltpu.VMEM((devices // 2, rows_two // 2, seeds), f32),
            pltpu.VMEM((devices // 2, rows_two // 2, seeds), bf16),
            pltpu.VMEM((devices // 2, rows_two // 2, seeds), bf16),
            pltpu.VMEM((devices // 16, rows_two // 2, seeds), bf16),
            pltpu.VMEM((devices // 16, rows_two // 2, seeds), bf16),
            pltpu.SemaphoreType.DMA((12,)),
            pltpu.SemaphoreType.DMA((2,)),
            pltpu.SemaphoreType.DMA((2, len(GROUPS) - 1)),
            pltpu.SemaphoreType.DMA((6,)),
            pltpu.SemaphoreType.DMA((devices // 16,)),
            pltpu.SemaphoreType.DMA((4,)),
            pltpu.SemaphoreType.DMA((4,)),
        ],
        compiler_params=pltpu.CompilerParams(
            vmem_limit_bytes=63 * MIB, collective_id=0, has_side_effects=True
        ),
    )(
        table_t,
        req_rows[:, None, :],
        req2_rows[:, None, :],
        count1,
        count2,
        frontier_list,
        seed_list,
        w1_self.T,
        w1_neigh.T,
        bias1[None, :],
        w2_self,
        w2_neigh,
    )
    return logits + bias2[:, None]


def solution(mesh):
    in_specs = (
        P(None, AXES),
        P(AXES, None),
        P(AXES),
        P(None, AXES),
        P(AXES, None),
        P(AXES),
        P(None, AXES),
        P(),
        P(),
        P(),
        P(),
        P(),
        P(),
    )
    return jax.shard_map(
        body, mesh=mesh, in_specs=in_specs, out_specs=P(None, AXES), check_vma=False
    )
```
